256 devices in a mesh: group: 16 (over z, x_lo), slot: 16 (over y, x_hi, core).
Axes of the slice: x: 4 (x_hi: 2, x_lo: 2; x = x_hi * 2 + x_lo), y: 4, z: 8, core: 2. Of those that a mesh axis runs over, the one named last changes fastest.
Arguments:
- rows_in: bfloat16 [131072, 768], P(('group', 'slot')), may hold values from -6 to 6
- cotangent: bfloat16 [131072, 2048], P(('group', 'slot')), may hold values from -6 to 6
- gate_prob: float32 [131072], P(('group', 'slot')), may hold values from 0.05 to 0.5
- row_counts: int32 [256], P(('group', 'slot')), may hold values from 1 to 512
- old_place: int32 [256, 1], replicated, may hold values from 0 to 63
- new_place: int32 [256, 1], replicated, may hold values from 0 to 63
- rows_next: bfloat16 [131072, 768], P(('group', 'slot')), may hold values from -6 to 6
- master: float32 [64, 768, 2048], P(None, 'slot', 'group'), may hold values from -0.21875 to 0.21875
- moment_one: bfloat16 [64, 768, 2048], P(None, 'slot', 'group'), may hold values from -18 to 18
- moment_two: bfloat16 [64, 768, 2048], P(None, 'slot', 'group'), may hold values from 0.049804688 to 2
Outputs:
- input_grad: bfloat16 [131072, 768], P(('group', 'slot'))
- gate_grad: float32 [131072], P(('group', 'slot'))
- new_master: float32 [64, 768, 2048], P(None, 'slot', 'group')
- new_first: bfloat16 [64, 768, 2048], P(None, 'slot', 'group')
- new_second: bfloat16 [64, 768, 2048], P(None, 'slot', 'group')
- next_out: bfloat16 [131072, 2048], P(('group', 'slot'))
The draws below stay inside these ranges and needn't reach their ends.
Inputs may be any that keep to these rules, and one draw needn't show every extreme that they name: `old_place`: every one of the 64 experts is held by at least one of the 256 slots. `new_place`: every one of the 64 experts is listed for at least one of the 256 slots.
All inputs are finite; a program needn't handle non-finite values.
Results may differ from the reference program's by a relative error of at most 0.004.
The reference program's roundings to bfloat16 on the way count: a program that leaves them out, or rounds other values in their place, can miss the bound.
Values may be sent and summed in bfloat16 or wider, within the bound.
A program may use at most 128 MiB of HBM per device.

```python
import math
import jax
import jax.numpy as jnp
from jax import lax

FF = 768
D = 2048
ROWS = 512
SLOTS = 256
EXPERTS = 64


def touch_ends(array, own_key, low, largest):
    longest = array.shape.index(max(array.shape))
    spots = []
    for shift in (0, 1):
        where = [jax.random.randint(jax.random.fold_in(own_key, axis), (), 0, length) for axis, length in enumerate(array.shape)]
        where[longest] = (where[longest] + shift) % array.shape[longest]
        spots.append(tuple(where))
    return array.at[spots[0]].set(low).at[spots[1]].set(largest)


def shard_levels(rng, extent, shards, low, high):
    factor_of, own = 1.0, jax.random.fold_in(rng, 6)
    for position, parts in shards:
        heights = jnp.exp(jax.random.uniform(jax.random.fold_in(own, position), (parts,), jnp.float32, low / len(shards), high / len(shards)))
        factor_of = factor_of * jnp.repeat(heights, extent[position] // parts).reshape([-1 if axis == position else 1 for axis in range(len(extent))])
    return factor_of


def choose_distinct(key, rows, number_of, top, lift):
    sequence = jax.random.permutation(jax.random.fold_in(key, 1), number_of)
    favour = sequence
    for power in range(3):
        favour = favour * favour // number_of
    favour = favour * lift // number_of
    chance = jax.random.randint(jax.random.fold_in(key, 2), (rows, number_of), 0, 4096) + favour
    fixed_rows = jax.random.permutation(jax.random.fold_in(key, 3), rows)[jnp.arange(number_of) % rows]
    chance = jnp.where(jnp.arange(rows)[:, None] == fixed_rows[None, :], 1 << 14, chance)
    merit = chance * number_of + jnp.arange(number_of)
    return lax.top_k(merit.astype(jnp.int32), top)[1].astype(jnp.int32)


def normal_values(rng, dims, spread, limit, cuts=(), kind=jnp.bfloat16):
    drawn = spread * jax.random.normal(rng, dims, jnp.float32)
    if cuts:
        drawn = drawn * shard_levels(rng, dims, cuts, -0.22, 0.18)
    return jnp.clip(drawn, -limit, limit).astype(kind)


def setup_inputs(seed: int = 0) -> dict:
    splits = jax.random.split(jax.random.key(seed), 11)
    return {
        "rows_in": normal_values(splits[0], (SLOTS * ROWS, FF), 1.0, 6.0, ((0, 256),)),
        "cotangent": normal_values(splits[1], (SLOTS * ROWS, D), 1.0, 6.0, ((0, 256),)),
        "gate_prob": jnp.clip(0.05 + 0.45 * jax.random.uniform(splits[2], (SLOTS * ROWS,), jnp.float32) ** shard_levels(splits[2], (SLOTS * ROWS,), ((0, 256),), -0.2, 0.2), 0.05, 0.5),
        "row_counts": touch_ends(jax.random.randint(splits[3], (SLOTS,), 1, ROWS + 1), jax.random.fold_in(splits[3], 1), 1, ROWS).astype(jnp.int32),
        "old_place": choose_distinct(splits[4], SLOTS, EXPERTS, 1, 256),
        "new_place": choose_distinct(splits[5], SLOTS, EXPERTS, 1, 256),
        "rows_next": normal_values(splits[6], (SLOTS * ROWS, FF), 1.0, 6.0, ((0, 256),)),
        "master": normal_values(splits[7], (EXPERTS, FF, D), FF ** -0.5, 0.21875, ((1, 16), (2, 16)), jnp.float32),
        "moment_one": normal_values(splits[8], (EXPERTS, FF, D), 3.0, 18.0, ((1, 16), (2, 16))),
        "moment_two": jnp.clip(jnp.exp(math.log(2.0) - 3.6927934 * jax.random.uniform(splits[9], (EXPERTS, FF, D), jnp.float32) ** shard_levels(splits[9], (EXPERTS, FF, D), ((1, 16), (2, 16)), -0.2, 0.2)), 0.049804688, 2.0).astype(jnp.bfloat16),
    }


beta_one = 0.9
beta_two = 0.999
adam_eps = 1e-08
learn_rate = 0.006
fix_one = 0.9999734386011124
fix_two = 0.0952078528862904

def reference(rows_in, cotangent, gate_prob, row_counts, old_place, new_place, rows_next, master, moment_one, moment_two):
    slot_rows = rows_in.reshape(SLOTS, ROWS, FF)
    slot_cot = cotangent.reshape(SLOTS, ROWS, D)
    slot_gate = gate_prob.reshape(SLOTS, ROWS)
    slot_next = rows_next.reshape(SLOTS, ROWS, FF)
    positions = jnp.arange(ROWS, dtype=jnp.int32)

    def run_slot(grad_sum, slot_item):
        inputs, upstream, gate_values, live_count, expert = slot_item
        live_rows = (positions < live_count)[:, None]
        masked_in = jnp.where(live_rows, inputs, jnp.zeros_like(inputs))
        masked_out = jnp.where(live_rows, upstream, jnp.zeros_like(upstream))
        weight = master[expert].astype(jnp.bfloat16)
        back_prod = jnp.dot(masked_out, weight.T, preferred_element_type=jnp.float32)
        input_grad = (gate_values[:, None] * back_prod).astype(jnp.bfloat16)
        forward_out = jnp.dot(masked_in, weight, preferred_element_type=jnp.float32)
        gate_grad = lax.optimization_barrier(jnp.sum(masked_out.astype(jnp.float32) * forward_out, axis=1))
        scaled_out = (gate_values[:, None] * masked_out.astype(jnp.float32)).astype(jnp.bfloat16)
        slot_grad = jnp.dot(masked_in.T, scaled_out, preferred_element_type=jnp.float32).astype(jnp.bfloat16)
        grad_sum = grad_sum.at[expert].add(slot_grad.astype(jnp.float32))
        return (grad_sum, (input_grad, gate_grad))
    zero_grad = jnp.zeros(master.shape, jnp.float32)
    grad_sum, (input_grad, gate_grad) = lax.scan(run_slot, zero_grad, (slot_rows, slot_cot, slot_gate, row_counts, old_place[:, 0]))
    first_full = beta_one * moment_one.astype(jnp.float32) + (1.0 - beta_one) * grad_sum
    second_full = beta_two * moment_two.astype(jnp.float32) + (1.0 - beta_two) * grad_sum * grad_sum
    new_master = master - learn_rate * (first_full / fix_one) / (jnp.sqrt(second_full / fix_two) + adam_eps)

    def run_next(slot_item):
        next_rows, expert = slot_item
        weight = new_master[expert].astype(jnp.bfloat16)
        return jnp.dot(next_rows, weight, preferred_element_type=jnp.float32).astype(jnp.bfloat16)
    next_out = lax.map(run_next, (slot_next, new_place[:, 0]))
    return (input_grad.reshape(SLOTS * ROWS, FF), gate_grad.reshape(SLOTS * ROWS), new_master, first_full.astype(jnp.bfloat16), second_full.astype(jnp.bfloat16), next_out.reshape(SLOTS * ROWS, D))
```

```python
import functools

import jax
import jax.numpy as jnp
from jax import lax
from jax.experimental import pallas as pl
from jax.experimental.pallas import tpu as pltpu
from jax.sharding import PartitionSpec as P

beta_one = 0.9
beta_two = 0.999
adam_eps = 1e-08
learn_rate = 0.006
fix_one = 0.9999734386011124
fix_two = 0.0952078528862904

EXPERTS = 64
PR = 48
PC = 128
PLANES = 8
INPLANE = 32
FAR = 80
MESH = pl.DeviceIdType.MESH

PREV_AT = 256
LAST_AT = PREV_AT + 2 * FAR
TABLE = LAST_AT + 3 * EXPERTS


def my_place():
    g = lax.axis_index("group")
    s = lax.axis_index("slot")
    z = lax.div(g, 2)
    return z, lax.rem(g, 2) * 16 + s, g, s


def plane_at(z, k):
    return lax.rem(z + (k + PLANES), PLANES)


def device_at(plane, i):
    return (plane * 2 + lax.div(i, 16), lax.rem(i, 16))


def shard_slice(ref, block_row, block_col):
    return ref.at[
        pl.ds(pl.multiple_of(block_row * PR, 16), PR), pl.ds(pl.multiple_of(block_col * PC, PC), PC)
    ]


def send(src, dst, send_sem, recv_sem, device):
    copy = pltpu.make_async_remote_copy(
        src_ref=src,
        dst_ref=dst,
        send_sem=send_sem,
        recv_sem=recv_sem,
        device_id=device,
        device_id_type=MESH,
    )
    copy.start()


def take(ref, sem):
    pltpu.make_async_copy(ref, ref, sem).wait()


class Spread:
    def __init__(self, place, own, weight, near, far, picks, ring_sems, out_sem, in_sems):
        self.place, self.own, self.weight = place, own, weight
        self.near, self.far, self.picks = near, far, picks
        self.ring_sems, self.out_sem, self.in_sems = ring_sems, out_sem, in_sems
        self.z, self.i, self.g, self.s = my_place()
        self.xlo = lax.rem(self.g, 2)

    def ring(self, src, dst, hop, side):
        send(
            src,
            dst,
            self.ring_sems.at[0, hop, side],
            self.ring_sems.at[1, hop, side],
            device_at(plane_at(self.z, 1 - 2 * side), self.i),
        )

    def start_own(self):
        for side in range(2):
            self.ring(self.own, self.near[side], 0, side)

    def wait_near(self, side):
        take(self.near[side], self.ring_sems.at[1, 0, side])

    def forward(self, side):
        self.ring(self.near[side], self.far[side], 1, side)

    def wait_far(self, side):
        take(self.far[side], self.ring_sems.at[1, 1, side])

    def inplane(self, ref, base, k):
        z, i = self.z, self.i
        column = plane_at(z, k) * 2 + self.xlo

        def pick(j, _):
            t = lax.rem(i + j, INPLANE)
            self.picks[base + j] = ref[self.place[z * INPLANE + t]]
            return 0

        def go(j, _):
            t = lax.rem(i + j, INPLANE)
            send(
                self.picks.at[base + j],
                shard_slice(self.weight, self.s, column),
                self.out_sem,
                self.in_sems.at[k + 3],
                device_at(z, t),
            )
            return 0

        lax.fori_loop(0, INPLANE, pick, 0)
        lax.fori_loop(1, INPLANE, go, 0)
        rows = pl.ds(pl.multiple_of(self.s * PR, 16), PR)
        cols = pl.ds(pl.multiple_of(column * PC, PC), PC)
        self.weight[rows, cols] = self.picks[base]

    def outplane(self, side, base):
        ref = self.far[side]
        sign = 1 - 2 * side
        z, i = self.z, self.i
        column = plane_at(z, -2 * sign) * 2 + self.xlo
        one, two = plane_at(z, sign), plane_at(z, 2 * sign)

        def other(j):
            return lax.rem((lax.div(i, 2) + j) * 2, INPLANE) + side

        def pick_one(j, _):
            t = lax.rem(i + j, INPLANE)
            self.picks[base + j] = ref[self.place[one * INPLANE + t]]
            return 0

        def pick_two(j, _):
            self.picks[base + 32 + j] = ref[self.place[two * INPLANE + other(j)]]
            return 0

        def go_one(j, _):
            t = lax.rem(i + j, INPLANE)
            send(
                self.picks.at[base + j],
                shard_slice(self.weight, self.s, column),
                self.out_sem,
                self.in_sems.at[3 - 3 * sign],
                device_at(one, t),
            )
            return 0

        def go_two(j, _):
            send(
                self.picks.at[base + 32 + j],
                shard_slice(self.weight, self.s, column),
                self.out_sem,
                self.in_sems.at[7],
                device_at(two, other(j)),
            )
            return 0

        lax.fori_loop(0, 16, pick_two, 0)
        lax.fori_loop(0, INPLANE, pick_one, 0)
        lax.fori_loop(0, 16, go_two, 0)
        lax.fori_loop(0, INPLANE, go_one, 0)

    def finish(self):
        for k in range(-3, 5):
            count = 31 if -2 <= k <= 2 else 32
            take(self.picks.at[pl.ds(0, count)], self.in_sems.at[k + 3])
        sent = 5 * 31 + 2 * 48
        take(self.picks.at[pl.ds(0, sent)], self.out_sem)
        for hop in range(2):
            for side in range(2):
                take(self.own, self.ring_sems.at[0, hop, side])


SPREAD_SCRATCH = [
    pltpu.VMEM((EXPERTS, PR, PC), jnp.bfloat16),
    pltpu.VMEM((EXPERTS, PR, PC), jnp.bfloat16),
    pltpu.VMEM((EXPERTS, PR, PC), jnp.bfloat16),
    pltpu.VMEM((EXPERTS, PR, PC), jnp.bfloat16),
    pltpu.VMEM((256, PR, PC), jnp.bfloat16),
    pltpu.SemaphoreType.DMA((2, 2, 2)),
    pltpu.SemaphoreType.DMA,
    pltpu.SemaphoreType.DMA((8,)),
]


class Gather:
    def __init__(self, table, grad, total, met0, met1, met2, sums, parts, sems, part_sems):
        self.table, self.grad, self.total = table, grad, total
        self.met0, self.met1, self.met2 = met0, met1, met2
        self.sums = sums
        self.parts = parts
        self.sems, self.part_sems = sems, part_sems
        self.z, self.i, self.g, self.s = my_place()
        self.out_sem = sems.at[0]

    def piece(self, plane, t):
        return shard_slice(self.grad, lax.rem(t, 16), plane * 2 + lax.div(t, 16))

    def piece_value(self, plane, t):
        rows = pl.ds(pl.multiple_of(lax.rem(t, 16) * PR, 16), PR)
        cols = pl.ds(pl.multiple_of((plane * 2 + lax.div(t, 16)) * PC, PC), PC)
        return self.grad[rows, cols]

    def start_far(self):
        z, i = self.z, self.i
        core = lax.rem(self.s, 2)
        two = lax.rem(z + 2 + 4 * core, PLANES)
        opposite = plane_at(z, 4)

        def go_two(j, _):
            t = lax.rem(i + j, INPLANE)
            send(
                self.piece(opposite, t),
                self.met2.at[core, 64 + lax.div(i, 2)],
                self.out_sem,
                self.sems.at[4 + core],
                device_at(two, t),
            )
            return 0

        def go_one(j, _):
            t = lax.rem(i + j, INPLANE)
            for side in range(2):
                sign = 1 - 2 * side
                send(
                    self.piece(plane_at(z, 3 * sign), t),
                    self.met2.at[side, 32 + i],
                    self.out_sem,
                    self.sems.at[4 + side],
                    device_at(plane_at(z, sign), t),
                )
            return 0

        lax.fori_loop(0, INPLANE, go_two, 0)
        lax.fori_loop(0, INPLANE, go_one, 0)

    def start_inplane(self):
        z, i = self.z, self.i

        def go(level, j):
            t = lax.rem(i + j, INPLANE)
            for side in range(2):
                sign = 1 - 2 * side
                met = self.met2 if level == 2 else self.met1
                send(
                    self.piece(plane_at(z, level * sign), t),
                    met.at[side, i],
                    self.out_sem,
                    self.sems.at[2 * level + side],
                    device_at(z, t),
                )
            return 0

        def go_own(j, _):
            t = lax.rem(i + j, INPLANE)
            send(self.piece(z, t), self.met0.at[i], self.out_sem, self.sems.at[1], device_at(z, t))
            return 0

        lax.fori_loop(1, INPLANE, lambda j, _: go(2, j), 0)
        lax.fori_loop(1, INPLANE, lambda j, _: go(1, j), 0)
        lax.fori_loop(1, INPLANE, go_own, 0)
        for side in range(2):
            sign = 1 - 2 * side
            self.met2[side, i] = self.piece_value(plane_at(z, 2 * sign), i)
            self.met1[side, i] = self.piece_value(plane_at(z, sign), i)
        self.met0[i] = self.piece_value(z, i)
        self.sums[...] = jnp.zeros_like(self.sums)

    def chain(self, value_at, count, side):
        def step(t, _):
            before = self.sums[self.table[PREV_AT + side * FAR + t]]
            self.sums[t] = before + value_at(t).astype(jnp.float32)
            return 0

        lax.fori_loop(0, count, step, 0)

    def summed(self, which, e):
        return self.sums[self.table[LAST_AT + which * EXPERTS + e]]

    def pass_on(self, level, side):
        sign = 1 - 2 * side
        send(
            self.parts[level].at[side],
            self.parts[2 + level].at[side],
            self.part_sems.at[0, level, side],
            self.part_sems.at[1, level, side],
            device_at(plane_at(self.z, sign), self.i),
        )

    def level_two(self, side):
        take(self.met2.at[side, pl.ds(0, FAR - 1)], self.sems.at[4 + side])
        self.chain(lambda t: self.met2[side, t], FAR, side)

        def put(e, _):
            self.parts[0][side, e] = self.summed(side, e).astype(jnp.bfloat16)
            return 0

        lax.fori_loop(0, EXPERTS, put, 0)
        self.pass_on(0, side)

    def level_one(self, side):
        take(self.met1.at[side, pl.ds(0, INPLANE - 1)], self.sems.at[2 + side])
        self.chain(lambda t: self.met1[side, t], INPLANE, 0)
        take(self.parts[2].at[side], self.part_sems.at[1, 0, side])

        def put(e, _):
            value = self.summed(2, e) + self.parts[2][side, e].astype(jnp.float32)
            self.parts[1][side, e] = value.astype(jnp.bfloat16)
            return 0

        lax.fori_loop(0, EXPERTS, put, 0)
        self.pass_on(1, side)

    def level_zero(self):
        take(self.met0.at[pl.ds(0, INPLANE - 1)], self.sems.at[1])
        self.chain(lambda t: self.met0[t], INPLANE, 0)
        for side in range(2):
            take(self.parts[3].at[side], self.part_sems.at[1, 1, side])

        def put(e, _):
            value = self.parts[3][0, e].astype(jnp.float32) + self.parts[3][1, e].astype(jnp.float32)
            self.total[e] = value + self.summed(2, e)
            return 0

        lax.fori_loop(0, EXPERTS, put, 0)

    def finish(self):
        take(self.met2.at[0], self.out_sem)
        take(self.met2.at[0], self.out_sem)
        take(self.met2.at[0], self.out_sem)
        take(self.met2.at[0, pl.ds(0, 5 * 31 + 96 - 3 * FAR)], self.out_sem)
        for level in range(2):
            for side in range(2):
                take(self.parts[level].at[side], self.part_sems.at[0, level, side])


GATHER_SCRATCH = [
    pltpu.VMEM((INPLANE, PR, PC), jnp.bfloat16),
    pltpu.VMEM((2, INPLANE, PR, PC), jnp.bfloat16),
    pltpu.VMEM((2, FAR, PR, PC), jnp.bfloat16),
    pltpu.VMEM((FAR + 1, PR, PC), jnp.float32),
    pltpu.VMEM((2, EXPERTS, PR, PC), jnp.bfloat16),
    pltpu.VMEM((2, EXPERTS, PR, PC), jnp.bfloat16),
    pltpu.VMEM((2, EXPERTS, PR, PC), jnp.bfloat16),
    pltpu.VMEM((2, EXPERTS, PR, PC), jnp.bfloat16),
    pltpu.SemaphoreType.DMA((6,)),
    pltpu.SemaphoreType.DMA((2, 2, 2)),
]


def first_kernel(table, own, grad, weight, total, *scratch):
    n = len(SPREAD_SCRATCH)
    near, far, picks = scratch[0:2], scratch[2:4], scratch[4]
    spread = Spread(table, own, weight, near, far, picks, *scratch[5:n])
    rest = scratch[n:]
    gather = Gather(table, grad, total, *rest[0:4], rest[4:8], *rest[8:])
    gather.start_far()
    spread.start_own()
    gather.start_inplane()
    spread.inplane(own, 0, 0)
    for side in range(2):
        gather.level_two(side)
    for side in range(2):
        spread.wait_near(side)
        spread.forward(side)
    for side in range(2):
        spread.inplane(near[side], 32 + 32 * side, -1 + 2 * side)
    for side in range(2):
        gather.level_one(side)
    for side in range(2):
        spread.wait_far(side)
        spread.outplane(side, 96 + 48 * side)
    for side in range(2):
        spread.inplane(far[side], 192 + 32 * side, -2 + 4 * side)
    gather.level_zero()
    spread.finish()
    gather.finish()


def second_kernel(table, own, weight, *scratch):
    near, far, picks = scratch[0:2], scratch[2:4], scratch[4]
    spread = Spread(table, own, weight, near, far, picks, *scratch[5:])
    spread.start_own()
    spread.inplane(own, 0, 0)
    for side in range(2):
        spread.wait_near(side)
        spread.forward(side)
    for side in range(2):
        spread.inplane(near[side], 32 + 32 * side, -1 + 2 * side)
    for side in range(2):
        spread.wait_far(side)
        spread.outplane(side, 96 + 48 * side)
    for side in range(2):
        spread.inplane(far[side], 192 + 32 * side, -2 + 4 * side)
    spread.finish()


VMEM = pl.BlockSpec(memory_space=pltpu.VMEM)
SMEM = pl.BlockSpec(memory_space=pltpu.SMEM)


def remote_call(kernel, operands, outs, scratch):
    return pl.pallas_call(
        kernel,
        out_shape=outs,
        in_specs=[SMEM] + [VMEM] * (len(operands) - 1),
        out_specs=tuple(VMEM for _ in outs),
        scratch_shapes=scratch,
        compiler_params=pltpu.CompilerParams(has_side_effects=True, vmem_limit_bytes=60 * 2**20),
    )(*operands)


def sum_tables(place, z):
    planes = place.reshape(PLANES, INPLANE)
    around = lax.dynamic_slice(
        jnp.concatenate([planes, planes], 0), (lax.rem(z + 6, PLANES), 0), (5, INPLANE)
    )
    up = jnp.concatenate([around[2], around[1], around[0].reshape(16, 2)[:, 0]])
    down = jnp.concatenate([around[2], around[3], around[4].reshape(16, 2)[:, 1]])
    both = jnp.stack([up, down])
    at = jnp.arange(FAR, dtype=jnp.int32)
    same = both[:, :, None] == both[:, None, :]
    earlier = at[None, :] < at[:, None]
    prev = jnp.max(jnp.where(same & earlier[None], at[None, None, :], -1), axis=2)
    prev = jnp.where(prev < 0, FAR, prev)
    lists = jnp.stack([up, down, jnp.where(at < INPLANE, up, -1)])
    ids = jnp.arange(EXPERTS, dtype=jnp.int32)
    found = lists[:, None, :] == ids[None, :, None]
    last = jnp.max(jnp.where(found, at[None, None, :], -1), axis=2)
    last = jnp.where(last < 0, FAR, last)
    return jnp.concatenate([place, prev.reshape(-1), last.reshape(-1)])


def shards(
    rows_in,
    cotangent,
    gate_prob,
    row_counts,
    old_place,
    new_place,
    rows_next,
    master,
    moment_one,
    moment_two,
):
    row_count = rows_in.shape[0]
    z = lax.div(lax.axis_index("group"), 2)
    live_rows = (jnp.arange(row_count, dtype=jnp.int32) < row_counts[0])[:, None]
    masked_in = jnp.where(live_rows, rows_in, jnp.zeros_like(rows_in))
    masked_out = jnp.where(live_rows, cotangent, jnp.zeros_like(cotangent))
    scaled_out = (gate_prob[:, None] * masked_out.astype(jnp.float32)).astype(jnp.bfloat16)
    slot_grad = lax.dot_general(
        masked_in, scaled_out, (((0,), (0,)), ((), ())), preferred_element_type=jnp.float32
    ).astype(jnp.bfloat16)
    weight_shape = jax.ShapeDtypeStruct((16 * PR, 16 * PC), jnp.bfloat16)
    table = sum_tables(old_place[:, 0], z)
    weight, grad_sum = remote_call(
        first_kernel,
        (table, master.astype(jnp.bfloat16), slot_grad),
        (weight_shape, jax.ShapeDtypeStruct(master.shape, jnp.float32)),
        SPREAD_SCRATCH + GATHER_SCRATCH,
    )
    first_full = beta_one * moment_one.astype(jnp.float32) + (1.0 - beta_one) * grad_sum
    second_full = beta_two * moment_two.astype(jnp.float32) + (1.0 - beta_two) * grad_sum * grad_sum
    new_master = master - learn_rate * (first_full / fix_one) / (
        jnp.sqrt(second_full / fix_two) + adam_eps
    )
    (weight_next,) = remote_call(
        second_kernel,
        (new_place[:, 0], new_master.astype(jnp.bfloat16)),
        (weight_shape,),
        SPREAD_SCRATCH,
    )
    back_prod = lax.dot_general(
        masked_out, weight, (((1,), (1,)), ((), ())), preferred_element_type=jnp.float32
    )
    input_grad = (gate_prob[:, None] * back_prod).astype(jnp.bfloat16)
    gate_grad = jnp.sum(masked_in.astype(jnp.float32) * back_prod, axis=1)
    next_out = jnp.dot(rows_next, weight_next, preferred_element_type=jnp.float32).astype(
        jnp.bfloat16
    )
    return (
        input_grad,
        gate_grad,
        new_master,
        first_full.astype(jnp.bfloat16),
        second_full.astype(jnp.bfloat16),
        next_out,
    )


def solution(mesh):
    in_specs = (
        P(("group", "slot"), None),
        P(("group", "slot"), None),
        P(("group", "slot")),
        P(("group", "slot")),
        P(),
        P(),
        P(("group", "slot"), None),
        P(None, "slot", "group"),
        P(None, "slot", "group"),
        P(None, "slot", "group"),
    )
    out_specs = (
        P(("group", "slot"), None),
        P(("group", "slot")),
        P(None, "slot", "group"),
        P(None, "slot", "group"),
        P(None, "slot", "group"),
        P(("group", "slot"), None),
    )
    return jax.shard_map(shards, mesh=mesh, in_specs=in_specs, out_specs=out_specs, check_vma=False)
```

```python
import functools

import jax
import jax.numpy as jnp
from jax import lax
from jax.experimental import pallas as pl
from jax.experimental.pallas import tpu as pltpu
from jax.sharding import PartitionSpec as P

beta_one = 0.9
beta_two = 0.999
adam_eps = 1e-08
learn_rate = 0.006
fix_one = 0.9999734386011124
fix_two = 0.0952078528862904

EXPERTS = 64
PR = 48
PC = 128
PLANES = 8
INPLANE = 32
FAR = 80
MESH = pl.DeviceIdType.MESH

PREV_AT = 256
LAST_AT = PREV_AT + 2 * FAR
TABLE = LAST_AT + 3 * EXPERTS


def my_place():
    g = lax.axis_index("group")
    s = lax.axis_index("slot")
    z = lax.div(g, 2)
    return z, lax.rem(g, 2) * 16 + s, g, s


def plane_at(z, k):
    return lax.rem(z + (k + PLANES), PLANES)


def device_at(plane, i):
    return (plane * 2 + lax.div(i, 16), lax.rem(i, 16))


def shard_slice(ref, block_row, block_col):
    return ref.at[
        pl.ds(pl.multiple_of(block_row * PR, 16), PR), pl.ds(pl.multiple_of(block_col * PC, PC), PC)
    ]


def send(src, dst, send_sem, recv_sem, device):
    copy = pltpu.make_async_remote_copy(
        src_ref=src,
        dst_ref=dst,
        send_sem=send_sem,
        recv_sem=recv_sem,
        device_id=device,
        device_id_type=MESH,
    )
    copy.start()


def take(ref, sem):
    pltpu.make_async_copy(ref, ref, sem).wait()


CHUNKS = 4
CE = EXPERTS // CHUNKS
PEERS = 5 * INPLANE - 1


def meet():
    z, i, _, _ = my_place()
    barrier = pltpu.get_barrier_semaphore()

    def go(n, _):
        m = PEERS - n
        k = lax.div(m, INPLANE)
        plane = lax.rem(z + k + 3 * lax.div(k, 3), PLANES)
        g, s = device_at(plane, lax.rem(i + m, INPLANE))
        pl.semaphore_signal(barrier, inc=1, device_id=(g, s), device_id_type=MESH)
        return 0

    lax.fori_loop(0, PEERS, go, 0)
    pl.semaphore_wait(barrier, PEERS)


class Spread:
    def __init__(self, place, base, own, weight, bufs):
        self.place, self.base, self.own, self.weight = place, base, own, weight
        self.near, self.far, self.picks = bufs[0:2], bufs[2:4], bufs[4]
        self.ring_sems, self.out_sem, self.in_sems = bufs[5:8]
        self.z, self.i, self.g, self.s = my_place()
        self.xlo = lax.rem(self.g, 2)

    def expert(self, plane, t):
        return self.place[self.base + plane * INPLANE + t]

    def ring(self, src, dst, hop, side, chunk):
        part = pl.ds(chunk * CE, CE)
        send(
            src.at[part],
            dst.at[part],
            self.ring_sems.at[0, hop, side, chunk],
            self.ring_sems.at[1, hop, side, chunk],
            device_at(plane_at(self.z, 1 - 2 * side), self.i),
        )

    def start_own(self, chunk):
        for side in range(2):
            self.ring(self.own, self.near[side], 0, side, chunk)

    def forward(self, chunk):
        for side in range(2):
            take(self.near[side].at[pl.ds(chunk * CE, CE)], self.ring_sems.at[1, 0, side, chunk])
            self.ring(self.near[side], self.far[side], 1, side, chunk)

    def wait_far(self):
        for chunk in range(CHUNKS):
            for side in range(2):
                take(self.far[side].at[pl.ds(chunk * CE, CE)], self.ring_sems.at[1, 1, side, chunk])

    def inplane(self, k):
        z, i = self.z, self.i
        ref = {0: self.own, -1: self.near[0], 1: self.near[1], -2: self.far[0], 2: self.far[1]}[k]
        base = {0: 0, -1: 32, 1: 64, -2: 192, 2: 224}[k]
        column = plane_at(z, k) * 2 + self.xlo

        def pick(j, _):
            t = lax.rem(i + j, INPLANE)
            self.picks[base + j] = ref[self.expert(z, t)]
            return 0

        def go(j, _):
            t = lax.rem(i + j, INPLANE)
            send(
                self.picks.at[base + j],
                shard_slice(self.weight, self.s, column),
                self.out_sem,
                self.in_sems.at[k + 3],
                device_at(z, t),
            )
            return 0

        lax.fori_loop(0, INPLANE, pick, 0)
        lax.fori_loop(1, INPLANE, go, 0)
        rows = pl.ds(pl.multiple_of(self.s * PR, 16), PR)
        cols = pl.ds(pl.multiple_of(column * PC, PC), PC)
        self.weight[rows, cols] = self.picks[base]

    def other(self, side, j):
        return lax.rem((lax.div(self.i, 2) + j) * 2, INPLANE) + side

    def pick_out(self, side):
        ref, base = self.far[side], 96 + 48 * side
        sign = 1 - 2 * side
        one, two = plane_at(self.z, sign), plane_at(self.z, 2 * sign)

        def pick_two(j, _):
            self.picks[base + 32 + j] = ref[self.expert(two, self.other(side, j))]
            return 0

        def pick_one(j, _):
            self.picks[base + j] = ref[self.expert(one, lax.rem(self.i + j, INPLANE))]
            return 0

        lax.fori_loop(0, 16, pick_two, 0)
        lax.fori_loop(0, INPLANE, pick_one, 0)

    def out_two(self):
        def go_two(j, _):
            for side in range(2):
                sign = 1 - 2 * side
                column = plane_at(self.z, -2 * sign) * 2 + self.xlo
                send(
                    self.picks.at[96 + 48 * side + 32 + j],
                    shard_slice(self.weight, self.s, column),
                    self.out_sem,
                    self.in_sems.at[7],
                    device_at(plane_at(self.z, 2 * sign), self.other(side, j)),
                )
            return 0

        lax.fori_loop(0, 16, go_two, 0)

    def out_one(self):
        def go_one(j, _):
            for side in range(2):
                sign = 1 - 2 * side
                column = plane_at(self.z, -2 * sign) * 2 + self.xlo
                send(
                    self.picks.at[96 + 48 * side + j],
                    shard_slice(self.weight, self.s, column),
                    self.out_sem,
                    self.in_sems.at[3 - 3 * sign],
                    device_at(plane_at(self.z, sign), lax.rem(self.i + j, INPLANE)),
                )
            return 0

        lax.fori_loop(0, INPLANE, go_one, 0)

    def arrived(self, k):
        count = 31 if -2 <= k <= 2 else 32
        take(self.picks.at[pl.ds(0, count)], self.in_sems.at[k + 3])

    def sent(self):
        take(self.picks.at[pl.ds(0, 5 * 31 + 2 * 48)], self.out_sem)
        for chunk in range(CHUNKS):
            for hop in range(2):
                for side in range(2):
                    part = self.own.at[pl.ds(chunk * CE, CE)]
                    take(part, self.ring_sems.at[0, hop, side, chunk])


SPREAD_SCRATCH = [
    pltpu.VMEM((EXPERTS, PR, PC), jnp.bfloat16),
    pltpu.VMEM((EXPERTS, PR, PC), jnp.bfloat16),
    pltpu.VMEM((EXPERTS, PR, PC), jnp.bfloat16),
    pltpu.VMEM((EXPERTS, PR, PC), jnp.bfloat16),
    pltpu.VMEM((256, PR, PC), jnp.bfloat16),
    pltpu.SemaphoreType.DMA((2, 2, 2, CHUNKS)),
    pltpu.SemaphoreType.DMA,
    pltpu.SemaphoreType.DMA((8,)),
]


class Gather:
    def __init__(self, table, grad, met0, met1, met2, sums, parts, sems, part_sems):
        self.table, self.grad = table, grad
        self.met0, self.met1, self.met2 = met0, met1, met2
        self.sums = sums
        self.parts = parts
        self.sems, self.part_sems = sems, part_sems
        self.z, self.i, self.g, self.s = my_place()
        self.out_sem = sems.at[0]

    def piece(self, plane, t):
        return shard_slice(self.grad, lax.rem(t, 16), plane * 2 + lax.div(t, 16))

    def piece_value(self, plane, t):
        rows = pl.ds(pl.multiple_of(lax.rem(t, 16) * PR, 16), PR)
        cols = pl.ds(pl.multiple_of((plane * 2 + lax.div(t, 16)) * PC, PC), PC)
        return self.grad[rows, cols]

    def start_far(self):
        z, i = self.z, self.i
        core = lax.rem(self.s, 2)
        two = lax.rem(z + 2 + 4 * core, PLANES)
        opposite = plane_at(z, 4)

        def go_two(j, _):
            t = lax.rem(i + j, INPLANE)
            send(
                self.piece(opposite, t),
                self.met2.at[core, 64 + lax.div(i, 2)],
                self.out_sem,
                self.sems.at[4 + core],
                device_at(two, t),
            )
            return 0

        def go_one(j, _):
            t = lax.rem(i + j, INPLANE)
            for side in range(2):
                sign = 1 - 2 * side
                send(
                    self.piece(plane_at(z, 3 * sign), t),
                    self.met2.at[side, 32 + i],
                    self.out_sem,
                    self.sems.at[4 + side],
                    device_at(plane_at(z, sign), t),
                )
            return 0

        lax.fori_loop(0, INPLANE, go_two, 0)
        lax.fori_loop(0, INPLANE, go_one, 0)

    def start_inplane(self):
        z, i = self.z, self.i

        def go(level, j):
            t = lax.rem(i + j, INPLANE)
            for side in range(2):
                sign = 1 - 2 * side
                met = self.met2 if level == 2 else self.met1
                send(
                    self.piece(plane_at(z, level * sign), t),
                    met.at[side, i],
                    self.out_sem,
                    self.sems.at[2 * level + side],
                    device_at(z, t),
                )
            return 0

        def go_own(j, _):
            t = lax.rem(i + j, INPLANE)
            send(self.piece(z, t), self.met0.at[i], self.out_sem, self.sems.at[1], device_at(z, t))
            return 0

        lax.fori_loop(1, INPLANE, lambda j, _: go(2, j), 0)
        lax.fori_loop(1, INPLANE, lambda j, _: go(1, j), 0)
        lax.fori_loop(1, INPLANE, go_own, 0)
        for side in range(2):
            sign = 1 - 2 * side
            self.met2[side, i] = self.piece_value(plane_at(z, 2 * sign), i)
            self.met1[side, i] = self.piece_value(plane_at(z, sign), i)
        self.met0[i] = self.piece_value(z, i)
        self.sums[...] = jnp.zeros_like(self.sums)

    def chain(self, value_at, count, side):
        def step(t, _):
            before = self.sums[self.table[PREV_AT + side * FAR + t]]
            self.sums[t] = before + value_at(t).astype(jnp.float32)
            return 0

        lax.fori_loop(0, count, step, 0)

    def summed(self, which, e):
        return self.sums[self.table[LAST_AT + which * EXPERTS + e]]

    def pass_on(self, level, side):
        sign = 1 - 2 * side
        send(
            self.parts[level].at[side],
            self.parts[2 + level].at[side],
            self.part_sems.at[0, level, side],
            self.part_sems.at[1, level, side],
            device_at(plane_at(self.z, sign), self.i),
        )

    def level_two(self, side):
        take(self.met2.at[side, pl.ds(0, FAR - 1)], self.sems.at[4 + side])
        self.chain(lambda t: self.met2[side, t], FAR, side)

        def put(e, _):
            self.parts[0][side, e] = self.summed(side, e).astype(jnp.bfloat16)
            return 0

        lax.fori_loop(0, EXPERTS, put, 0)
        self.pass_on(0, side)

    def level_one(self, side):
        take(self.met1.at[side, pl.ds(0, INPLANE - 1)], self.sems.at[2 + side])
        self.chain(lambda t: self.met1[side, t], INPLANE, 0)
        take(self.parts[2].at[side], self.part_sems.at[1, 0, side])

        def put(e, _):
            value = self.summed(2, e) + self.parts[2][side, e].astype(jnp.float32)
            self.parts[1][side, e] = value.astype(jnp.bfloat16)
            return 0

        lax.fori_loop(0, EXPERTS, put, 0)
        self.pass_on(1, side)

    def level_zero(self):
        take(self.met0.at[pl.ds(0, INPLANE - 1)], self.sems.at[1])
        self.chain(lambda t: self.met0[t], INPLANE, 0)
        for side in range(2):
            take(self.parts[3].at[side], self.part_sems.at[1, 1, side])

    def total(self, e):
        value = self.parts[3][0, e].astype(jnp.float32) + self.parts[3][1, e].astype(jnp.float32)
        return value + self.summed(2, e)

    def finish(self):
        take(self.met2.at[0], self.out_sem)
        take(self.met2.at[0], self.out_sem)
        take(self.met2.at[0], self.out_sem)
        take(self.met2.at[0, pl.ds(0, 5 * 31 + 96 - 3 * FAR)], self.out_sem)
        for level in range(2):
            for side in range(2):
                take(self.parts[level].at[side], self.part_sems.at[0, level, side])


GATHER_SCRATCH = [
    pltpu.VMEM((INPLANE, PR, PC), jnp.bfloat16),
    pltpu.VMEM((2, INPLANE, PR, PC), jnp.bfloat16),
    pltpu.VMEM((2, FAR, PR, PC), jnp.bfloat16),
    pltpu.VMEM((FAR + 1, PR, PC), jnp.float32),
    pltpu.VMEM((2, EXPERTS, PR, PC), jnp.bfloat16),
    pltpu.VMEM((2, EXPERTS, PR, PC), jnp.bfloat16),
    pltpu.VMEM((2, EXPERTS, PR, PC), jnp.bfloat16),
    pltpu.VMEM((2, EXPERTS, PR, PC), jnp.bfloat16),
    pltpu.SemaphoreType.DMA((6,)),
    pltpu.SemaphoreType.DMA((2, 2, 2)),
]


STATE = (EXPERTS, PR, PC)
STATE_SCRATCH = [
    pltpu.VMEM(STATE, jnp.float32),
    pltpu.VMEM(STATE, jnp.bfloat16),
    pltpu.VMEM(STATE, jnp.bfloat16),
    pltpu.VMEM(STATE, jnp.bfloat16),
    pltpu.VMEM(STATE, jnp.bfloat16),
    pltpu.SemaphoreType.DMA((6,)),
]


def step_kernel(
    table,
    grad,
    master_in,
    first_in,
    second_in,
    weight,
    weight_next,
    master_out,
    first_out,
    second_out,
    *scratch,
):
    n = len(SPREAD_SCRATCH)
    m = len(GATHER_SCRATCH)
    master, first, second, own, own_next, state_sems = scratch[2 * n + m :]
    now = Spread(table, 0, own, weight, scratch[0:n])
    after = Spread(table, TABLE, own_next, weight_next, scratch[n : 2 * n])
    rest = scratch[2 * n : 2 * n + m]
    gather = Gather(table, grad, *rest[0:4], rest[4:8], *rest[8:])

    loads = [
        pltpu.make_async_copy(src, dst, state_sems.at[at])
        for at, (src, dst) in enumerate(((master_in, master), (first_in, first), (second_in, second)))
    ]
    for load in loads:
        load.start()
    meet()
    loads[0].wait()

    def cast(e, _):
        own[e] = master[e].astype(jnp.bfloat16)
        return 0

    lax.fori_loop(0, EXPERTS, cast, 0)
    gather.start_far()
    for chunk in range(CHUNKS):
        now.start_own(chunk)
    gather.start_inplane()
    now.inplane(0)
    now.forward(0)
    now.forward(1)
    for side in range(2):
        gather.level_two(side)
    now.forward(2)
    now.forward(3)
    now.inplane(-1)
    now.inplane(1)
    for side in range(2):
        gather.level_one(side)
    now.wait_far()
    for side in range(2):
        now.pick_out(side)
    now.out_two()
    now.inplane(-2)
    now.inplane(2)
    gather.level_zero()
    for load in loads[1:]:
        load.wait()

    def update(e, _):
        grad_sum = gather.total(e)
        first_full = beta_one * first[e].astype(jnp.float32) + (1.0 - beta_one) * grad_sum
        second_full = (
            beta_two * second[e].astype(jnp.float32) + (1.0 - beta_two) * grad_sum * grad_sum
        )
        moved = master[e] - learn_rate * (first_full / fix_one) / (
            jnp.sqrt(second_full / fix_two) + adam_eps
        )
        master[e] = moved
        own_next[e] = moved.astype(jnp.bfloat16)
        first[e] = first_full.astype(jnp.bfloat16)
        second[e] = second_full.astype(jnp.bfloat16)
        return 0

    for chunk in range(CHUNKS):
        lax.fori_loop(chunk * CE, (chunk + 1) * CE, update, 0)
        after.start_own(chunk)
    stores = [
        pltpu.make_async_copy(src, dst, state_sems.at[3 + at])
        for at, (src, dst) in enumerate(
            ((master, master_out), (first, first_out), (second, second_out))
        )
    ]
    for store in stores:
        store.start()
    after.inplane(0)
    for chunk in range(CHUNKS):
        after.forward(chunk)
    now.out_one()
    after.inplane(-1)
    after.inplane(1)
    after.wait_far()
    for side in range(2):
        after.pick_out(side)
    after.out_two()
    after.out_one()
    after.inplane(-2)
    after.inplane(2)
    for k in range(-3, 5):
        now.arrived(k)
    for store in stores:
        store.wait()
    now.sent()
    gather.finish()
    for k in range(-3, 5):
        after.arrived(k)
    after.sent()


ANY = pl.BlockSpec(memory_space=pl.ANY)
VMEM = pl.BlockSpec(memory_space=pltpu.VMEM)
SMEM = pl.BlockSpec(memory_space=pltpu.SMEM)


def step_call(table, grad, master, moment_one, moment_two):
    weight = jax.ShapeDtypeStruct((16 * PR, 16 * PC), jnp.bfloat16)
    return pl.pallas_call(
        step_kernel,
        out_shape=(
            weight,
            weight,
            jax.ShapeDtypeStruct(STATE, jnp.float32),
            jax.ShapeDtypeStruct(STATE, jnp.bfloat16),
            jax.ShapeDtypeStruct(STATE, jnp.bfloat16),
        ),
        in_specs=[SMEM, VMEM, ANY, ANY, ANY],
        out_specs=(VMEM, VMEM, ANY, ANY, ANY),
        scratch_shapes=SPREAD_SCRATCH * 2 + GATHER_SCRATCH + STATE_SCRATCH,
        compiler_params=pltpu.CompilerParams(
            has_side_effects=True, collective_id=0, vmem_limit_bytes=60 * 2**20
        ),
    )(table, grad, master, moment_one, moment_two)


def sum_tables(place, z):
    planes = place.reshape(PLANES, INPLANE)
    around = lax.dynamic_slice(
        jnp.concatenate([planes, planes], 0), (lax.rem(z + 6, PLANES), 0), (5, INPLANE)
    )
    up = jnp.concatenate([around[2], around[1], around[0].reshape(16, 2)[:, 0]])
    down = jnp.concatenate([around[2], around[3], around[4].reshape(16, 2)[:, 1]])
    both = jnp.stack([up, down])
    at = jnp.arange(FAR, dtype=jnp.int32)
    same = both[:, :, None] == both[:, None, :]
    earlier = at[None, :] < at[:, None]
    prev = jnp.max(jnp.where(same & earlier[None], at[None, None, :], -1), axis=2)
    prev = jnp.where(prev < 0, FAR, prev)
    lists = jnp.stack([up, down, jnp.where(at < INPLANE, up, -1)])
    ids = jnp.arange(EXPERTS, dtype=jnp.int32)
    found = lists[:, None, :] == ids[None, :, None]
    last = jnp.max(jnp.where(found, at[None, None, :], -1), axis=2)
    last = jnp.where(last < 0, FAR, last)
    return prev.reshape(-1), last.reshape(-1)


def shards(
    rows_in,
    cotangent,
    gate_prob,
    row_counts,
    old_place,
    new_place,
    rows_next,
    master,
    moment_one,
    moment_two,
):
    row_count = rows_in.shape[0]
    z = lax.div(lax.axis_index("group"), 2)
    live_rows = (jnp.arange(row_count, dtype=jnp.int32) < row_counts[0])[:, None]
    masked_in = jnp.where(live_rows, rows_in, jnp.zeros_like(rows_in))
    masked_out = jnp.where(live_rows, cotangent, jnp.zeros_like(cotangent))
    scaled_out = (gate_prob[:, None] * masked_out.astype(jnp.float32)).astype(jnp.bfloat16)
    slot_grad = lax.dot_general(
        masked_in, scaled_out, (((0,), (0,)), ((), ())), preferred_element_type=jnp.float32
    ).astype(jnp.bfloat16)
    old, new = old_place.reshape(-1), new_place.reshape(-1)
    table = jnp.concatenate([old, *sum_tables(old, z), new])
    weight, weight_next, new_master, new_first, new_second = step_call(
        table, slot_grad, master, moment_one, moment_two
    )
    back_prod = lax.dot_general(
        masked_out, weight, (((1,), (1,)), ((), ())), preferred_element_type=jnp.float32
    )
    input_grad = (gate_prob[:, None] * back_prod).astype(jnp.bfloat16)
    gate_grad = jnp.sum(masked_in.astype(jnp.float32) * back_prod, axis=1)
    next_out = jnp.dot(rows_next, weight_next, preferred_element_type=jnp.float32).astype(
        jnp.bfloat16
    )
    return (
        input_grad,
        gate_grad,
        new_master,
        new_first,
        new_second,
        next_out,
    )


def solution(mesh):
    in_specs = (
        P(("group", "slot"), None),
        P(("group", "slot"), None),
        P(("group", "slot")),
        P(("group", "slot")),
        P(),
        P(),
        P(("group", "slot"), None),
        P(None, "slot", "group"),
        P(None, "slot", "group"),
        P(None, "slot", "group"),
    )
    out_specs = (
        P(("group", "slot"), None),
        P(("group", "slot")),
        P(None, "slot", "group"),
        P(None, "slot", "group"),
        P(None, "slot", "group"),
        P(("group", "slot"), None),
    )
    return jax.shard_map(shards, mesh=mesh, in_specs=in_specs, out_specs=out_specs, check_vma=False)
```

```python
import jax
import jax.numpy as jnp
from jax import lax
from jax.experimental import pallas as pl
from jax.experimental.pallas import tpu as pltpu
from jax.sharding import PartitionSpec as P

beta_one = 0.9
beta_two = 0.999
adam_eps = 1e-08
learn_rate = 0.006
fix_one = 0.9999734386011124
fix_two = 0.0952078528862904

EXPERTS = 64
PR = 48
PC = 128
PLANES = 8
INPLANE = 32
FAR = 80
MESH = pl.DeviceIdType.MESH


def my_place():
    g = lax.axis_index("group")
    s = lax.axis_index("slot")
    z = lax.div(g, 2)
    return z, lax.rem(g, 2) * 16 + s, g, s


def plane_at(z, k):
    return lax.rem(z + (k + PLANES), PLANES)


def device_at(plane, i):
    return (plane * 2 + lax.div(i, 16), lax.rem(i, 16))


def shard_slice(ref, block_row, block_col):
    return ref.at[
        pl.ds(pl.multiple_of(block_row * PR, 16), PR), pl.ds(pl.multiple_of(block_col * PC, PC), PC)
    ]


def send(src, dst, send_sem, recv_sem, device):
    copy = pltpu.make_async_remote_copy(
        src_ref=src,
        dst_ref=dst,
        send_sem=send_sem,
        recv_sem=recv_sem,
        device_id=device,
        device_id_type=MESH,
    )
    copy.start()


def take(ref, sem):
    pltpu.make_async_copy(ref, ref, sem).wait()


CHUNKS = 4
PARTS = ((0, 32), (32, 16))
PEERS = 5 * INPLANE - 1


def meet():
    z, i, _, _ = my_place()
    barrier = pltpu.get_barrier_semaphore()

    def go(n, _):
        m = PEERS - n
        k = lax.div(m, INPLANE)
        plane = lax.rem(z + k + 3 * lax.div(k, 3), PLANES)
        g, s = device_at(plane, lax.rem(i + m, INPLANE))
        pl.semaphore_signal(barrier, inc=1, device_id=(g, s), device_id_type=MESH)
        return 0

    lax.fori_loop(0, PEERS, go, 0)
    return barrier


class Spread:
    def __init__(self, place, own, weight, first_row, chunks, bufs):
        self.place, self.own, self.weight = place, own, weight
        self.first_row, self.count = first_row, own.shape[1]
        self.chunks, self.step = chunks, EXPERTS // chunks
        self.near, self.far, self.picks = bufs[0:2], bufs[2:4], bufs[4]
        self.ring_sems, self.out_sem, self.in_sems = bufs[5:8]
        self.z, self.i, self.g, self.s = my_place()
        self.xlo = lax.rem(self.g, 2)

    def expert(self, plane, t):
        return self.place[plane * INPLANE + t]

    def ring(self, src, dst, hop, side, chunk):
        part = pl.ds(chunk * self.step, self.step)
        send(
            src.at[part],
            dst.at[part],
            self.ring_sems.at[0, hop, side, chunk],
            self.ring_sems.at[1, hop, side, chunk],
            device_at(plane_at(self.z, 1 - 2 * side), self.i),
        )

    def start_own(self, chunk):
        for side in range(2):
            self.ring(self.own, self.near[side], 0, side, chunk)

    def forward(self, chunk):
        for side in range(2):
            part = self.near[side].at[pl.ds(chunk * self.step, self.step)]
            take(part, self.ring_sems.at[1, 0, side, chunk])
            self.ring(self.near[side], self.far[side], 1, side, chunk)

    def wait_far(self):
        for chunk in range(self.chunks):
            for side in range(2):
                part = self.far[side].at[pl.ds(chunk * self.step, self.step)]
                take(part, self.ring_sems.at[1, 1, side, chunk])

    def span(self):
        return pl.ds(pl.multiple_of(self.s * PR + self.first_row, 16), self.count)

    def target(self, column):
        return self.weight.at[self.span(), pl.ds(pl.multiple_of(column * PC, PC), PC)]

    def inplane(self, k):
        z, i = self.z, self.i
        ref = {0: self.own, -1: self.near[0], 1: self.near[1], -2: self.far[0], 2: self.far[1]}[k]
        base = {0: 0, -1: 32, 1: 64, -2: 192, 2: 224}[k]
        column = plane_at(z, k) * 2 + self.xlo

        def pick(j, _):
            t = lax.rem(i + j, INPLANE)
            self.picks[base + j] = ref[self.expert(z, t)]
            return 0

        def go(j, _):
            t = lax.rem(i + j, INPLANE)
            send(
                self.picks.at[base + j],
                self.target(column),
                self.out_sem,
                self.in_sems.at[k + 3],
                device_at(z, t),
            )
            return 0

        lax.fori_loop(0, INPLANE, pick, 0)
        lax.fori_loop(1, INPLANE, go, 0)
        self.weight[self.span(), pl.ds(pl.multiple_of(column * PC, PC), PC)] = self.picks[base]

    def other(self, side, j):
        return lax.rem((lax.div(self.i, 2) + j) * 2, INPLANE) + side

    def pick_out(self, side):
        ref, base = self.far[side], 96 + 48 * side
        sign = 1 - 2 * side
        one, two = plane_at(self.z, sign), plane_at(self.z, 2 * sign)

        def pick_two(j, _):
            self.picks[base + 32 + j] = ref[self.expert(two, self.other(side, j))]
            return 0

        def pick_one(j, _):
            self.picks[base + j] = ref[self.expert(one, lax.rem(self.i + j, INPLANE))]
            return 0

        lax.fori_loop(0, 16, pick_two, 0)
        lax.fori_loop(0, INPLANE, pick_one, 0)

    def out_two(self):
        def go_two(j, _):
            for side in range(2):
                sign = 1 - 2 * side
                column = plane_at(self.z, -2 * sign) * 2 + self.xlo
                send(
                    self.picks.at[96 + 48 * side + 32 + j],
                    self.target(column),
                    self.out_sem,
                    self.in_sems.at[7],
                    device_at(plane_at(self.z, 2 * sign), self.other(side, j)),
                )
            return 0

        lax.fori_loop(0, 16, go_two, 0)

    def out_one(self):
        def go_one(j, _):
            for side in range(2):
                sign = 1 - 2 * side
                column = plane_at(self.z, -2 * sign) * 2 + self.xlo
                send(
                    self.picks.at[96 + 48 * side + j],
                    self.target(column),
                    self.out_sem,
                    self.in_sems.at[3 - 3 * sign],
                    device_at(plane_at(self.z, sign), lax.rem(self.i + j, INPLANE)),
                )
            return 0

        lax.fori_loop(0, INPLANE, go_one, 0)

    def arrived(self, k):
        count = 31 if -2 <= k <= 2 else 32
        take(self.picks.at[pl.ds(0, count)], self.in_sems.at[k + 3])

    def sent(self):
        take(self.picks.at[pl.ds(0, 5 * 31 + 2 * 48)], self.out_sem)
        for chunk in range(self.chunks):
            for hop in range(2):
                for side in range(2):
                    part = self.own.at[pl.ds(chunk * self.step, self.step)]
                    take(part, self.ring_sems.at[0, hop, side, chunk])


def spread_scratch(rows, chunks):
    shards = [pltpu.VMEM((EXPERTS, rows, PC), jnp.bfloat16) for _ in range(4)]
    return shards + [
        pltpu.VMEM((256, rows, PC), jnp.bfloat16),
        pltpu.SemaphoreType.DMA((2, 2, 2, chunks)),
        pltpu.SemaphoreType.DMA,
        pltpu.SemaphoreType.DMA((8,)),
    ]


class Gather:
    def __init__(self, prev, last, grad, met0, met1, met2, sums, parts, sems, part_sems):
        self.prev, self.last, self.grad = prev, last, grad
        self.met0, self.met1, self.met2 = met0, met1, met2
        self.sums = sums
        self.parts = parts
        self.sems, self.part_sems = sems, part_sems
        self.z, self.i, self.g, self.s = my_place()
        self.out_sem = sems.at[0]

    def piece(self, plane, t):
        return shard_slice(self.grad, lax.rem(t, 16), plane * 2 + lax.div(t, 16))

    def piece_value(self, plane, t):
        rows = pl.ds(pl.multiple_of(lax.rem(t, 16) * PR, 16), PR)
        cols = pl.ds(pl.multiple_of((plane * 2 + lax.div(t, 16)) * PC, PC), PC)
        return self.grad[rows, cols]

    def start_far(self):
        z, i = self.z, self.i
        core = lax.rem(self.s, 2)
        two = lax.rem(z + 2 + 4 * core, PLANES)
        opposite = plane_at(z, 4)

        def go_two(j, _):
            t = lax.rem(i + j, INPLANE)
            send(
                self.piece(opposite, t),
                self.met2.at[core, 64 + lax.div(i, 2)],
                self.out_sem,
                self.sems.at[4 + core],
                device_at(two, t),
            )
            return 0

        def go_one(j, _):
            t = lax.rem(i + j, INPLANE)
            for side in range(2):
                sign = 1 - 2 * side
                send(
                    self.piece(plane_at(z, 3 * sign), t),
                    self.met2.at[side, 32 + i],
                    self.out_sem,
                    self.sems.at[4 + side],
                    device_at(plane_at(z, sign), t),
                )
            return 0

        lax.fori_loop(0, INPLANE, go_two, 0)
        lax.fori_loop(0, INPLANE, go_one, 0)

    def start_inplane(self, level):
        z, i = self.z, self.i

        def go(level, j):
            t = lax.rem(i + j, INPLANE)
            for side in range(2):
                sign = 1 - 2 * side
                met = self.met2 if level == 2 else self.met1
                send(
                    self.piece(plane_at(z, level * sign), t),
                    met.at[side, i],
                    self.out_sem,
                    self.sems.at[2 * level + side],
                    device_at(z, t),
                )
            return 0

        def go_own(j, _):
            t = lax.rem(i + j, INPLANE)
            send(self.piece(z, t), self.met0.at[i], self.out_sem, self.sems.at[1], device_at(z, t))
            return 0

        if level == 0:
            lax.fori_loop(1, INPLANE, go_own, 0)
            self.met0[i] = self.piece_value(z, i)
            return
        lax.fori_loop(1, INPLANE, lambda j, _: go(level, j), 0)
        met = self.met2 if level == 2 else self.met1
        for side in range(2):
            met[side, i] = self.piece_value(plane_at(z, level * (1 - 2 * side)), i)

    def chain(self, value_at, count, side):
        def step(t, _):
            before = self.sums[self.prev[side * FAR + t]]
            self.sums[t] = before + value_at(t).astype(jnp.float32)
            return 0

        lax.fori_loop(0, count, step, 0)

    def summed(self, which, e):
        return self.sums[self.last[which * EXPERTS + e]]

    def clear(self):
        self.sums[...] = jnp.zeros_like(self.sums)

    def pass_on(self, level, side):
        sign = 1 - 2 * side
        send(
            self.parts[level].at[side],
            self.parts[2 + level].at[side],
            self.part_sems.at[0, level, side],
            self.part_sems.at[1, level, side],
            device_at(plane_at(self.z, sign), self.i),
        )

    def level_two(self, side):
        take(self.met2.at[side, pl.ds(0, FAR - 1)], self.sems.at[4 + side])
        self.chain(lambda t: self.met2[side, t], FAR, side)

        def put(e, _):
            self.parts[0][side, e] = self.summed(side, e).astype(jnp.bfloat16)
            return 0

        lax.fori_loop(0, EXPERTS, put, 0)
        self.pass_on(0, side)

    def level_one(self, side):
        take(self.met1.at[side, pl.ds(0, INPLANE - 1)], self.sems.at[2 + side])
        self.chain(lambda t: self.met1[side, t], INPLANE, 0)
        take(self.parts[2].at[side], self.part_sems.at[1, 0, side])

        def put(e, _):
            value = self.summed(2, e) + self.parts[2][side, e].astype(jnp.float32)
            self.parts[1][side, e] = value.astype(jnp.bfloat16)
            return 0

        lax.fori_loop(0, EXPERTS, put, 0)
        self.pass_on(1, side)

    def level_zero(self):
        take(self.met0.at[pl.ds(0, INPLANE - 1)], self.sems.at[1])
        self.chain(lambda t: self.met0[t], INPLANE, 0)
        for side in range(2):
            take(self.parts[3].at[side], self.part_sems.at[1, 1, side])

    def total(self, e, rows):
        value = self.parts[3][0, e, rows].astype(jnp.float32)
        value = value + self.parts[3][1, e, rows].astype(jnp.float32)
        return value + self.sums[self.last[2 * EXPERTS + e], rows]

    def finish(self):
        take(self.met2.at[0], self.out_sem)
        take(self.met2.at[0], self.out_sem)
        take(self.met2.at[0], self.out_sem)
        take(self.met2.at[0, pl.ds(0, 5 * 31 + 96 - 3 * FAR)], self.out_sem)
        for level in range(2):
            for side in range(2):
                take(self.parts[level].at[side], self.part_sems.at[0, level, side])


GATHER_SCRATCH = [
    pltpu.VMEM((INPLANE, PR, PC), jnp.bfloat16),
    pltpu.VMEM((2, INPLANE, PR, PC), jnp.bfloat16),
    pltpu.VMEM((2, FAR, PR, PC), jnp.bfloat16),
    pltpu.VMEM((FAR + 1, PR, PC), jnp.float32),
    pltpu.VMEM((2, EXPERTS, PR, PC), jnp.bfloat16),
    pltpu.VMEM((2, EXPERTS, PR, PC), jnp.bfloat16),
    pltpu.VMEM((2, EXPERTS, PR, PC), jnp.bfloat16),
    pltpu.VMEM((2, EXPERTS, PR, PC), jnp.bfloat16),
    pltpu.SemaphoreType.DMA((6,)),
    pltpu.SemaphoreType.DMA((2, 2, 2)),
]


STATE = (EXPERTS, PR, PC)
ROWS = 512
FF = 16 * PR
D = 16 * PC
BLOCK = 128
WIDE = 2 * PC
LOCAL_SCRATCH = [
    pltpu.VMEM(STATE, jnp.bfloat16),
    *[pltpu.VMEM((EXPERTS, rows, PC), jnp.bfloat16) for _, rows in PARTS],
    pltpu.VMEM((FF, D), jnp.bfloat16),
    pltpu.VMEM((FF, D), jnp.bfloat16),
    pltpu.VMEM((ROWS, FF), jnp.bfloat16),
    pltpu.VMEM((FF, ROWS), jnp.bfloat16),
    pltpu.VMEM((ROWS, D), jnp.bfloat16),
    pltpu.VMEM((ROWS, D), jnp.bfloat16),
    pltpu.VMEM((ROWS, BLOCK), jnp.float32),
    pltpu.SemaphoreType.DMA((5,)),
]


SCRATCHES = [spread_scratch(PR, CHUNKS)] + [spread_scratch(rows, 1) for _, rows in PARTS]

def step_kernel(
    old,
    new,
    prev,
    last,
    count,
    gate_in,
    rows_in,
    cot_in,
    master_in,
    first_in,
    second_in,
    weight_next,
    master,
    first,
    second,
    input_grad,
    gate_grad,
    *scratch,
):
    n = len(SCRATCHES[0])
    m = len(GATHER_SCRATCH)
    own, own_a, own_b, grad, weight, rows, rows_t, cot, scaled, gate, load_sems = scratch[3 * n + m :]
    now = Spread(old, own, weight, 0, CHUNKS, scratch[0:n])
    after = [
        Spread(new, part, weight_next, PARTS[at][0], 1, scratch[(at + 1) * n : (at + 2) * n])
        for at, part in enumerate((own_a, own_b))
    ]
    rest = scratch[3 * n : 3 * n + m]
    gather = Gather(prev, last, grad, *rest[0:4], rest[4:8], *rest[8:])
    z = now.z

    pairs = (
        (master_in, master),
        (rows_in, rows),
        (cot_in, cot),
        (first_in, first),
        (second_in, second),
    )
    loads = [
        pltpu.make_async_copy(src, dst, load_sems.at[at]) for at, (src, dst) in enumerate(pairs)
    ]
    for load in loads:
        load.start()
    barrier = meet()
    loads[0].wait()

    def cast(e, _):
        own[e] = master[e].astype(jnp.bfloat16)
        return 0

    lax.fori_loop(0, EXPERTS, cast, 0)
    pl.semaphore_wait(barrier, PEERS)
    for chunk in range(CHUNKS):
        now.start_own(chunk)

    now.inplane(0)
    loads[1].wait()
    loads[2].wait()
    live_count = count[0]
    for block in range(ROWS // BLOCK):
        at = pl.ds(block * BLOCK, BLOCK)
        live = lax.broadcasted_iota(jnp.int32, (BLOCK, BLOCK), 0) + block * BLOCK < live_count
        factor = jnp.transpose(jnp.broadcast_to(gate_in[block : block + 1, :], (BLOCK, BLOCK)))
        gate[at, :] = factor

        def mask_rows(c, _, at=at, live=live):
            cols = pl.ds(pl.multiple_of(c * BLOCK, BLOCK), BLOCK)
            value = jnp.where(live, rows[at, cols].astype(jnp.float32), 0.0)
            rows[at, cols] = value.astype(jnp.bfloat16)
            rows_t[cols, at] = jnp.transpose(value).astype(jnp.bfloat16)
            return 0

        def mask_cot(c, _, at=at, live=live, factor=factor):
            cols = pl.ds(pl.multiple_of(c * BLOCK, BLOCK), BLOCK)
            value = jnp.where(live, cot[at, cols].astype(jnp.float32), 0.0)
            cot[at, cols] = value.astype(jnp.bfloat16)
            scaled[at, cols] = (factor * value).astype(jnp.bfloat16)
            return 0

        lax.fori_loop(0, FF // BLOCK, mask_rows, 0)
        lax.fori_loop(0, D // BLOCK, mask_cot, 0)

    def slot_grad(p, _):
        half = lax.div(p + 1, 2)
        plane = lax.rem(z + 4 + (1 - 2 * lax.rem(p, 2)) * half, PLANES)
        cols = pl.ds(pl.multiple_of(plane * WIDE, WIDE), WIDE)
        grad[:, cols] = jnp.dot(
            rows_t[...], scaled[:, cols], preferred_element_type=jnp.float32
        ).astype(jnp.bfloat16)
        return 0

    lax.fori_loop(0, PLANES, slot_grad, 0)
    gather.clear()
    gather.start_far()
    gather.start_inplane(2)
    now.forward(0)
    now.forward(1)
    for side in range(2):
        gather.level_two(side)
    gather.start_inplane(1)
    gather.start_inplane(0)
    now.forward(2)
    now.forward(3)
    now.inplane(-1)
    now.inplane(1)
    for side in range(2):
        gather.level_one(side)
    now.wait_far()
    for side in range(2):
        now.pick_out(side)
    now.out_two()
    now.inplane(-2)
    now.inplane(2)
    gather.level_zero()
    for load in loads[3:]:
        load.wait()

    def update(e, rows, own_next):
        grad_sum = gather.total(e, rows)
        first_full = beta_one * first[e, rows].astype(jnp.float32) + (1.0 - beta_one) * grad_sum
        second_full = (
            beta_two * second[e, rows].astype(jnp.float32)
            + (1.0 - beta_two) * grad_sum * grad_sum
        )
        moved = master[e, rows] - learn_rate * (first_full / fix_one) / (
            jnp.sqrt(second_full / fix_two) + adam_eps
        )
        master[e, rows] = moved
        own_next[e] = moved.astype(jnp.bfloat16)
        first[e, rows] = first_full.astype(jnp.bfloat16)
        second[e, rows] = second_full.astype(jnp.bfloat16)
        return 0

    for at, part in enumerate(after):
        rows_at = pl.ds(*PARTS[at])
        lax.fori_loop(
            0, EXPERTS, lambda e, _, rows_at=rows_at, part=part: update(e, rows_at, part.own), 0
        )
        part.start_own(0)
    for part in after:
        part.inplane(0)
    for part in after:
        part.forward(0)
        part.inplane(-1)
        part.inplane(1)
    now.out_one()
    for part in after:
        part.wait_far()
        for side in range(2):
            part.pick_out(side)
        part.inplane(-2)
        part.inplane(2)
        part.out_two()
        part.out_one()
    for k in range(-3, 5):
        now.arrived(k)

    def back(block, _):
        at = pl.ds(pl.multiple_of(block * BLOCK, BLOCK), BLOCK)
        prod = lax.dot_general(
            cot[at, :], weight[...], (((1,), (1,)), ((), ())), preferred_element_type=jnp.float32
        )
        factor = gate[at, :]
        across = jnp.zeros((BLOCK, BLOCK), jnp.float32)
        for c in range(FF // BLOCK):
            part = prod[:, c * BLOCK : (c + 1) * BLOCK]
            cols = pl.ds(c * BLOCK, BLOCK)
            input_grad[at, cols] = (factor * part).astype(jnp.bfloat16)
            across = across + rows[at, cols].astype(jnp.float32) * part
        column = jnp.sum(across, axis=1, keepdims=True)
        turned = jnp.transpose(jnp.broadcast_to(column, (BLOCK, BLOCK)))
        gate_grad[pl.ds(block, 1), :] = turned[0:1, :]
        return 0

    lax.fori_loop(0, ROWS // BLOCK, back, 0)
    now.sent()
    gather.finish()
    for part in after:
        for k in range(-3, 5):
            part.arrived(k)
        part.sent()


def last_kernel(
    rows_next,
    weight,
    master,
    first,
    second,
    input_grad,
    next_out,
    master_out,
    first_out,
    second_out,
    input_out,
    out,
    sems,
):
    pairs = (
        (master, master_out),
        (first, first_out),
        (second, second_out),
        (input_grad, input_out),
    )
    stores = [pltpu.make_async_copy(src, dst, sems.at[at]) for at, (src, dst) in enumerate(pairs)]
    for store in stores:
        store.start()
    for block in range(ROWS // BLOCK):
        at = pl.ds(block * BLOCK, BLOCK)
        out[at, :] = jnp.dot(
            rows_next[at, :], weight[...], preferred_element_type=jnp.float32
        ).astype(jnp.bfloat16)
        stores.append(
            pltpu.make_async_copy(out.at[at], next_out.at[at], sems.at[len(pairs) + block])
        )
        stores[-1].start()
    for store in stores:
        store.wait()


ANY = pl.BlockSpec(memory_space=pl.ANY)
HBM = pl.BlockSpec(memory_space=pltpu.HBM)
VMEM = pl.BlockSpec(memory_space=pltpu.VMEM)
SMEM = pl.BlockSpec(memory_space=pltpu.SMEM)


def in_hbm(x):
    return pltpu.with_memory_space_constraint(x, pltpu.HBM)


def step_call(*operands):
    return pl.pallas_call(
        step_kernel,
        out_shape=(
            jax.ShapeDtypeStruct((FF, D), jnp.bfloat16),
            jax.ShapeDtypeStruct(STATE, jnp.float32),
            jax.ShapeDtypeStruct(STATE, jnp.bfloat16),
            jax.ShapeDtypeStruct(STATE, jnp.bfloat16),
            jax.ShapeDtypeStruct((ROWS, FF), jnp.bfloat16),
            jax.ShapeDtypeStruct((ROWS // BLOCK, BLOCK), jnp.float32),
        ),
        in_specs=[SMEM] * 5 + [VMEM] + [HBM] * 5,
        out_specs=(VMEM,) * 6,
        scratch_shapes=sum(SCRATCHES, []) + GATHER_SCRATCH + LOCAL_SCRATCH,
        compiler_params=pltpu.CompilerParams(
            has_side_effects=True, collective_id=0, vmem_limit_bytes=STEP_VMEM
        ),
    )(*operands)


STEP_VMEM = 39 * 2**20


def last_call(*operands):
    shapes = (
        jax.ShapeDtypeStruct((ROWS, D), jnp.bfloat16),
        jax.ShapeDtypeStruct(STATE, jnp.float32),
        jax.ShapeDtypeStruct(STATE, jnp.bfloat16),
        jax.ShapeDtypeStruct(STATE, jnp.bfloat16),
        jax.ShapeDtypeStruct((ROWS, FF), jnp.bfloat16),
    )
    return pl.pallas_call(
        last_kernel,
        out_shape=shapes,
        in_specs=[VMEM] * 6,
        out_specs=(ANY,) * 5,
        scratch_shapes=[pltpu.VMEM((ROWS, D), jnp.bfloat16), pltpu.SemaphoreType.DMA((8,))],
        compiler_params=pltpu.CompilerParams(vmem_limit_bytes=16 * 2**20),
    )(*operands)


def sum_tables(place, z):
    planes = place.reshape(PLANES, INPLANE)
    around = lax.dynamic_slice(
        jnp.concatenate([planes, planes], 0), (lax.rem(z + 6, PLANES), 0), (5, INPLANE)
    )
    up = jnp.concatenate([around[2], around[1], around[0].reshape(16, 2)[:, 0]])
    down = jnp.concatenate([around[2], around[3], around[4].reshape(16, 2)[:, 1]])
    both = jnp.stack([up, down])
    at = jnp.arange(FAR, dtype=jnp.int32)
    same = both[:, :, None] == both[:, None, :]
    earlier = at[None, :] < at[:, None]
    prev = jnp.max(jnp.where(same & earlier[None], at[None, None, :], -1), axis=2)
    prev = jnp.where(prev < 0, FAR, prev)
    lists = jnp.stack([up, down, jnp.where(at < INPLANE, up, -1)])
    ids = jnp.arange(EXPERTS, dtype=jnp.int32)
    found = lists[:, None, :] == ids[None, :, None]
    last = jnp.max(jnp.where(found, at[None, None, :], -1), axis=2)
    last = jnp.where(last < 0, FAR, last)
    return prev.reshape(-1), last.reshape(-1)


def shards(
    rows_in,
    cotangent,
    gate_prob,
    row_counts,
    old_place,
    new_place,
    rows_next,
    master,
    moment_one,
    moment_two,
):
    z = lax.div(lax.axis_index("group"), 2)
    old, new = old_place.reshape(-1), new_place.reshape(-1)
    prev, last = sum_tables(old, z)
    weight_next, new_master, new_first, new_second, input_grad, gate_grad = step_call(
        in_hbm(old),
        in_hbm(new),
        prev,
        last,
        row_counts,
        gate_prob.reshape(ROWS // BLOCK, BLOCK),
        in_hbm(rows_in),
        in_hbm(cotangent),
        in_hbm(master),
        in_hbm(moment_one),
        in_hbm(moment_two),
    )
    next_out, new_master, new_first, new_second, input_grad = last_call(
        rows_next, weight_next, new_master, new_first, new_second, input_grad
    )
    return (input_grad, gate_grad.reshape(-1), new_master, new_first, new_second, next_out)


def solution(mesh):
    in_specs = (
        P(("group", "slot"), None),
        P(("group", "slot"), None),
        P(("group", "slot")),
        P(("group", "slot")),
        P(),
        P(),
        P(("group", "slot"), None),
        P(None, "slot", "group"),
        P(None, "slot", "group"),
        P(None, "slot", "group"),
    )
    out_specs = (
        P(("group", "slot"), None),
        P(("group", "slot")),
        P(None, "slot", "group"),
        P(None, "slot", "group"),
        P(None, "slot", "group"),
        P(("group", "slot"), None),
    )
    return jax.shard_map(shards, mesh=mesh, in_specs=in_specs, out_specs=out_specs, check_vma=False)
```

```python
import jax
import jax.numpy as jnp
from jax import lax
from jax.experimental import pallas as pl
from jax.experimental.pallas import tpu as pltpu
from jax.sharding import PartitionSpec as P

beta_one = 0.9
beta_two = 0.999
adam_eps = 1e-08
learn_rate = 0.006
fix_one = 0.9999734386011124
fix_two = 0.0952078528862904

EXPERTS = 64
PR = 48
PC = 128
PLANES = 8
INPLANE = 32
FAR = 80
MESH = pl.DeviceIdType.MESH


def my_place():
    g = lax.axis_index("group")
    s = lax.axis_index("slot")
    z = lax.div(g, 2)
    return z, lax.rem(g, 2) * 16 + s, g, s


def plane_at(z, k):
    return lax.rem(z + (k + PLANES), PLANES)


def device_at(plane, i):
    return (plane * 2 + lax.div(i, 16), lax.rem(i, 16))


def shard_slice(ref, block_row, block_col):
    return ref.at[
        pl.ds(pl.multiple_of(block_row * PR, 16), PR), pl.ds(pl.multiple_of(block_col * PC, PC), PC)
    ]


def send(src, dst, send_sem, recv_sem, device):
    copy = pltpu.make_async_remote_copy(
        src_ref=src,
        dst_ref=dst,
        send_sem=send_sem,
        recv_sem=recv_sem,
        device_id=device,
        device_id_type=MESH,
    )
    copy.start()


def take(ref, sem):
    pltpu.make_async_copy(ref, ref, sem).wait()


CHUNKS = 4
PARTS = ((0, 32), (32, 16))
PEERS = 5 * INPLANE - 1


def meet():
    z, _, g, s = my_place()
    barrier = pltpu.get_barrier_semaphore()
    for k in (2, -2, 1, -1, 0):
        for half in range(2):
            group = plane_at(z, k) * 2 + lax.rem(g + half, 2)

            def go(j, _, group=group):
                pl.semaphore_signal(
                    barrier,
                    inc=1,
                    device_id=(group, lax.rem(s + j, 16)),
                    device_id_type=MESH,
                )
                return 0

            lax.fori_loop(1 if (k, half) == (0, 0) else 0, 16, go, 0)
    return barrier


class Spread:
    def __init__(self, place, own, weight, first_row, chunks, bufs):
        self.place, self.own, self.weight = place, own, weight
        self.first_row, self.count = first_row, own.shape[1]
        self.chunks, self.step = chunks, EXPERTS // chunks
        self.near, self.far, self.picks = bufs[0:2], bufs[2:4], bufs[4]
        self.ring_sems, self.out_sem, self.in_sems = bufs[5:8]
        self.z, self.i, self.g, self.s = my_place()
        self.xlo = lax.rem(self.g, 2)

    def expert(self, plane, t):
        return self.place[plane * INPLANE + t]

    def ring(self, src, dst, hop, side, chunk):
        part = pl.ds(chunk * self.step, self.step)
        send(
            src.at[part],
            dst.at[part],
            self.ring_sems.at[0, hop, side, chunk],
            self.ring_sems.at[1, hop, side, chunk],
            device_at(plane_at(self.z, 1 - 2 * side), self.i),
        )

    def start_own(self, chunk):
        for side in range(2):
            self.ring(self.own, self.near[side], 0, side, chunk)

    def forward(self, chunk):
        for side in range(2):
            part = self.near[side].at[pl.ds(chunk * self.step, self.step)]
            take(part, self.ring_sems.at[1, 0, side, chunk])
            self.ring(self.near[side], self.far[side], 1, side, chunk)

    def wait_far(self):
        for chunk in range(self.chunks):
            for side in range(2):
                part = self.far[side].at[pl.ds(chunk * self.step, self.step)]
                take(part, self.ring_sems.at[1, 1, side, chunk])

    def span(self):
        return pl.ds(pl.multiple_of(self.s * PR + self.first_row, 16), self.count)

    def target(self, column):
        return self.weight.at[self.span(), pl.ds(pl.multiple_of(column * PC, PC), PC)]

    def inplane(self, k):
        z, i = self.z, self.i
        ref = {0: self.own, -1: self.near[0], 1: self.near[1], -2: self.far[0], 2: self.far[1]}[k]
        base = {0: 0, -1: 32, 1: 64, -2: 192, 2: 224}[k]
        column = plane_at(z, k) * 2 + self.xlo

        def pick(j, _):
            t = lax.rem(i + j, INPLANE)
            self.picks[base + j] = ref[self.expert(z, t)]
            return 0

        def go(j, _):
            t = lax.rem(i + j, INPLANE)
            send(
                self.picks.at[base + j],
                self.target(column),
                self.out_sem,
                self.in_sems.at[k + 3],
                device_at(z, t),
            )
            return 0

        lax.fori_loop(0, INPLANE, pick, 0)
        lax.fori_loop(1, INPLANE, go, 0)
        self.weight[self.span(), pl.ds(pl.multiple_of(column * PC, PC), PC)] = self.picks[base]

    def other(self, side, j):
        return lax.rem((lax.div(self.i, 2) + j) * 2, INPLANE) + side

    def pick_out(self, side):
        ref, base = self.far[side], 96 + 48 * side
        sign = 1 - 2 * side
        one, two = plane_at(self.z, sign), plane_at(self.z, 2 * sign)

        def pick_two(j, _):
            self.picks[base + 32 + j] = ref[self.expert(two, self.other(side, j))]
            return 0

        def pick_one(j, _):
            self.picks[base + j] = ref[self.expert(one, lax.rem(self.i + j, INPLANE))]
            return 0

        lax.fori_loop(0, 16, pick_two, 0)
        lax.fori_loop(0, INPLANE, pick_one, 0)

    def out_two(self):
        def go_two(j, _):
            for side in range(2):
                sign = 1 - 2 * side
                column = plane_at(self.z, -2 * sign) * 2 + self.xlo
                send(
                    self.picks.at[96 + 48 * side + 32 + j],
                    self.target(column),
                    self.out_sem,
                    self.in_sems.at[7],
                    device_at(plane_at(self.z, 2 * sign), self.other(side, j)),
                )
            return 0

        lax.fori_loop(0, 16, go_two, 0)

    def out_one(self):
        def go_one(j, _):
            for side in range(2):
                sign = 1 - 2 * side
                column = plane_at(self.z, -2 * sign) * 2 + self.xlo
                send(
                    self.picks.at[96 + 48 * side + j],
                    self.target(column),
                    self.out_sem,
                    self.in_sems.at[3 - 3 * sign],
                    device_at(plane_at(self.z, sign), lax.rem(self.i + j, INPLANE)),
                )
            return 0

        lax.fori_loop(0, INPLANE, go_one, 0)

    def arrived(self, k):
        count = 31 if -2 <= k <= 2 else 32
        take(self.picks.at[pl.ds(0, count)], self.in_sems.at[k + 3])

    def sent(self):
        take(self.picks.at[pl.ds(0, 5 * 31 + 2 * 48)], self.out_sem)
        for chunk in range(self.chunks):
            for hop in range(2):
                for side in range(2):
                    part = self.own.at[pl.ds(chunk * self.step, self.step)]
                    take(part, self.ring_sems.at[0, hop, side, chunk])


def spread_scratch(rows, chunks):
    shards = [pltpu.VMEM((EXPERTS, rows, PC), jnp.bfloat16) for _ in range(4)]
    return shards + [
        pltpu.VMEM((256, rows, PC), jnp.bfloat16),
        pltpu.SemaphoreType.DMA((2, 2, 2, chunks)),
        pltpu.SemaphoreType.DMA,
        pltpu.SemaphoreType.DMA((8,)),
    ]


def build_tables(old, tab):
    z, _, _, _ = my_place()
    lanes = lax.broadcasted_iota(jnp.int32, (8, 128), 1)

    def near(t, lists):
        out = []
        for value, k in zip(lists, (-1, 1)):
            value = jnp.where(lanes == t, old[z * INPLANE + t], value)
            out.append(jnp.where(lanes == 32 + t, old[plane_at(z, k) * INPLANE + t], value))
        return tuple(out)

    def far(t, lists):
        out = []
        for core, (value, k) in enumerate(zip(lists, (-2, 2))):
            expert = old[plane_at(z, k) * INPLANE + 2 * t + core]
            out.append(jnp.where(lanes == 64 + t, expert, value))
        return tuple(out)

    none = jnp.full((8, 128), -1, jnp.int32)
    lists = lax.fori_loop(0, 16, far, lax.fori_loop(0, INPLANE, near, (none, none)))
    at = lax.broadcasted_iota(jnp.int32, (128, 128), 0)
    across = lax.broadcasted_iota(jnp.int32, (128, 128), 1)

    def put(row, found):
        value = jnp.where(found, at, -1)
        size = 128
        while size > 1:
            size //= 2
            value = jnp.maximum(value[:size], value[size:])
        tab[row : row + 1, :] = jnp.where(value < 0, FAR, value)

    for side in range(2):
        wide = jnp.broadcast_to(lists[side][0:1, :], (128, 128))
        tall = jnp.transpose(wide)
        put(side, (tall == wide) & (at < across))
        put(2 + side, tall == across)
        if side == 0:
            put(4, (tall == across) & (at < INPLANE))


class Gather:
    def __init__(self, tab, grad, met0, met1, met2, sums, parts, sems, part_sems):
        self.tab, self.grad = tab, grad
        self.met0, self.met1, self.met2 = met0, met1, met2
        self.sums = sums
        self.parts = parts
        self.sems, self.part_sems = sems, part_sems
        self.z, self.i, self.g, self.s = my_place()
        self.out_sem = sems.at[0]

    def piece(self, plane, t):
        return shard_slice(self.grad, lax.rem(t, 16), plane * 2 + lax.div(t, 16))

    def piece_value(self, plane, t):
        rows = pl.ds(pl.multiple_of(lax.rem(t, 16) * PR, 16), PR)
        cols = pl.ds(pl.multiple_of((plane * 2 + lax.div(t, 16)) * PC, PC), PC)
        return self.grad[rows, cols]

    def start_far(self):
        z, i = self.z, self.i
        core = lax.rem(self.s, 2)
        two = lax.rem(z + 2 + 4 * core, PLANES)
        opposite = plane_at(z, 4)

        def go_two(j, _):
            t = lax.rem(i + j, INPLANE)
            send(
                self.piece(opposite, t),
                self.met2.at[core, 64 + lax.div(i, 2)],
                self.out_sem,
                self.sems.at[4 + core],
                device_at(two, t),
            )
            return 0

        def go_one(j, _):
            t = lax.rem(i + j, INPLANE)
            for side in range(2):
                sign = 1 - 2 * side
                send(
                    self.piece(plane_at(z, 3 * sign), t),
                    self.met2.at[side, 32 + i],
                    self.out_sem,
                    self.sems.at[4 + side],
                    device_at(plane_at(z, sign), t),
                )
            return 0

        lax.fori_loop(0, INPLANE, go_two, 0)
        lax.fori_loop(0, INPLANE, go_one, 0)

    def start_inplane(self, level):
        z, i = self.z, self.i

        def go(level, j):
            t = lax.rem(i + j, INPLANE)
            for side in range(2):
                sign = 1 - 2 * side
                met = self.met2 if level == 2 else self.met1
                send(
                    self.piece(plane_at(z, level * sign), t),
                    met.at[side, i],
                    self.out_sem,
                    self.sems.at[2 * level + side],
                    device_at(z, t),
                )
            return 0

        def go_own(j, _):
            t = lax.rem(i + j, INPLANE)
            send(self.piece(z, t), self.met0.at[i], self.out_sem, self.sems.at[1], device_at(z, t))
            return 0

        if level == 0:
            lax.fori_loop(1, INPLANE, go_own, 0)
            self.met0[i] = self.piece_value(z, i)
            return
        lax.fori_loop(1, INPLANE, lambda j, _: go(level, j), 0)
        met = self.met2 if level == 2 else self.met1
        for side in range(2):
            met[side, i] = self.piece_value(plane_at(z, level * (1 - 2 * side)), i)

    def chain(self, value_at, count, side):
        def step(t, _):
            before = self.sums[self.tab[side, t]]
            self.sums[t] = before + value_at(t).astype(jnp.float32)
            return 0

        lax.fori_loop(0, count, step, 0)

    def summed(self, which, e):
        return self.sums[self.tab[2 + which, e]]

    def clear(self):
        self.sums[...] = jnp.zeros_like(self.sums)

    def pass_on(self, level, side):
        sign = 1 - 2 * side
        send(
            self.parts[level].at[side],
            self.parts[2 + level].at[side],
            self.part_sems.at[0, level, side],
            self.part_sems.at[1, level, side],
            device_at(plane_at(self.z, sign), self.i),
        )

    def level_two(self, side):
        take(self.met2.at[side, pl.ds(0, FAR - 1)], self.sems.at[4 + side])
        self.chain(lambda t: self.met2[side, t], FAR, side)

        def put(e, _):
            self.parts[0][side, e] = self.summed(side, e).astype(jnp.bfloat16)
            return 0

        lax.fori_loop(0, EXPERTS, put, 0)
        self.pass_on(0, side)

    def level_one(self, side):
        take(self.met1.at[side, pl.ds(0, INPLANE - 1)], self.sems.at[2 + side])
        self.chain(lambda t: self.met1[side, t], INPLANE, 0)
        take(self.parts[2].at[side], self.part_sems.at[1, 0, side])

        def put(e, _):
            value = self.summed(2, e) + self.parts[2][side, e].astype(jnp.float32)
            self.parts[1][side, e] = value.astype(jnp.bfloat16)
            return 0

        lax.fori_loop(0, EXPERTS, put, 0)
        self.pass_on(1, side)

    def level_zero(self):
        take(self.met0.at[pl.ds(0, INPLANE - 1)], self.sems.at[1])
        self.chain(lambda t: self.met0[t], INPLANE, 0)
        for side in range(2):
            take(self.parts[3].at[side], self.part_sems.at[1, 1, side])

    def total(self, e, rows):
        value = self.parts[3][0, e, rows].astype(jnp.float32)
        value = value + self.parts[3][1, e, rows].astype(jnp.float32)
        return value + self.sums[self.tab[4, e], rows]

    def finish(self):
        take(self.met2.at[0], self.out_sem)
        take(self.met2.at[0], self.out_sem)
        take(self.met2.at[0], self.out_sem)
        take(self.met2.at[0, pl.ds(0, 5 * 31 + 96 - 3 * FAR)], self.out_sem)
        for level in range(2):
            for side in range(2):
                take(self.parts[level].at[side], self.part_sems.at[0, level, side])


GATHER_SCRATCH = [
    pltpu.VMEM((INPLANE, PR, PC), jnp.bfloat16),
    pltpu.VMEM((2, INPLANE, PR, PC), jnp.bfloat16),
    pltpu.VMEM((2, FAR, PR, PC), jnp.bfloat16),
    pltpu.VMEM((FAR + 1, PR, PC), jnp.float32),
    pltpu.VMEM((2, EXPERTS, PR, PC), jnp.bfloat16),
    pltpu.VMEM((2, EXPERTS, PR, PC), jnp.bfloat16),
    pltpu.VMEM((2, EXPERTS, PR, PC), jnp.bfloat16),
    pltpu.VMEM((2, EXPERTS, PR, PC), jnp.bfloat16),
    pltpu.SemaphoreType.DMA((6,)),
    pltpu.SemaphoreType.DMA((2, 2, 2)),
]


STATE = (EXPERTS, PR, PC)
ROWS = 512
FF = 16 * PR
D = 16 * PC
BLOCK = 128
WIDE = 2 * PC
LOCAL_SCRATCH = [
    pltpu.VMEM(STATE, jnp.bfloat16),
    *[pltpu.VMEM((EXPERTS, rows, PC), jnp.bfloat16) for _, rows in PARTS],
    pltpu.VMEM((ROWS // BLOCK, BLOCK), jnp.float32),
    pltpu.VMEM((FF, D), jnp.bfloat16),
    pltpu.VMEM((FF, D), jnp.bfloat16),
    pltpu.VMEM((ROWS, FF), jnp.bfloat16),
    pltpu.VMEM((FF, ROWS), jnp.bfloat16),
    pltpu.VMEM((ROWS, D), jnp.bfloat16),
    pltpu.VMEM((ROWS, D), jnp.bfloat16),
    pltpu.VMEM((ROWS, BLOCK), jnp.float32),
    pltpu.SemaphoreType.DMA((7,)),
    pltpu.VMEM((8, 128), jnp.int32),
    pltpu.SMEM((8, 128), jnp.int32),
]


SCRATCHES = [spread_scratch(PR, CHUNKS)] + [spread_scratch(rows, 1) for _, rows in PARTS]

def step_kernel(
    old,
    new,
    count,
    gate_hbm,
    rows_in,
    cot_in,
    master_in,
    first_in,
    second_in,
    weight_next,
    master,
    first,
    second,
    input_grad,
    gate_grad,
    *scratch,
):
    n = len(SCRATCHES[0])
    m = len(GATHER_SCRATCH)
    own, own_a, own_b, gate_in, grad, weight, rows, rows_t, cot, scaled, gate, load_sems, tab, tab_smem = (
        scratch[3 * n + m :]
    )
    now = Spread(old, own, weight, 0, CHUNKS, scratch[0:n])
    after = [
        Spread(new, part, weight_next, PARTS[at][0], 1, scratch[(at + 1) * n : (at + 2) * n])
        for at, part in enumerate((own_a, own_b))
    ]
    rest = scratch[3 * n : 3 * n + m]
    gather = Gather(tab_smem, grad, *rest[0:4], rest[4:8], *rest[8:])
    z = now.z

    barrier = meet()
    pairs = (
        (master_in, master),
        (rows_in, rows),
        (cot_in, cot),
        (first_in, first),
        (second_in, second),
        (gate_hbm, gate_in),
    )
    loads = [
        pltpu.make_async_copy(src, dst, load_sems.at[at]) for at, (src, dst) in enumerate(pairs)
    ]
    for load in loads:
        load.start()
    loads[0].wait()

    def cast(e, _):
        own[e] = master[e].astype(jnp.bfloat16)
        return 0

    lax.fori_loop(0, EXPERTS, cast, 0)
    pl.semaphore_wait(barrier, PEERS)
    for chunk in range(CHUNKS):
        now.start_own(chunk)

    now.inplane(0)
    build_tables(old, tab)
    loads[1].wait()
    loads[2].wait()
    loads[5].wait()
    live_count = count[0]
    for block in range(ROWS // BLOCK):
        at = pl.ds(block * BLOCK, BLOCK)
        live = lax.broadcasted_iota(jnp.int32, (BLOCK, BLOCK), 0) + block * BLOCK < live_count
        factor = jnp.transpose(jnp.broadcast_to(gate_in[block : block + 1, :], (BLOCK, BLOCK)))
        gate[at, :] = factor

        def mask_rows(c, _, at=at, live=live):
            cols = pl.ds(pl.multiple_of(c * BLOCK, BLOCK), BLOCK)
            value = jnp.where(live, rows[at, cols].astype(jnp.float32), 0.0)
            rows[at, cols] = value.astype(jnp.bfloat16)
            rows_t[cols, at] = jnp.transpose(value).astype(jnp.bfloat16)
            return 0

        def mask_cot(c, _, at=at, live=live, factor=factor):
            cols = pl.ds(pl.multiple_of(c * BLOCK, BLOCK), BLOCK)
            value = jnp.where(live, cot[at, cols].astype(jnp.float32), 0.0)
            cot[at, cols] = value.astype(jnp.bfloat16)
            scaled[at, cols] = (factor * value).astype(jnp.bfloat16)
            return 0

        lax.fori_loop(0, FF // BLOCK, mask_rows, 0)
        lax.fori_loop(0, D // BLOCK, mask_cot, 0)

    def slot_grad(p, _):
        half = lax.div(p + 1, 2)
        plane = lax.rem(z + 4 + (1 - 2 * lax.rem(p, 2)) * half, PLANES)
        cols = pl.ds(pl.multiple_of(plane * WIDE, WIDE), WIDE)
        grad[:, cols] = jnp.dot(
            rows_t[...], scaled[:, cols], preferred_element_type=jnp.float32
        ).astype(jnp.bfloat16)
        return 0

    lax.fori_loop(0, PLANES, slot_grad, 0)
    gather.clear()
    gather.start_far()
    gather.start_inplane(2)
    tables = pltpu.make_async_copy(tab, tab_smem, load_sems.at[6])
    tables.start()
    tables.wait()
    now.forward(0)
    now.forward(1)
    for side in range(2):
        gather.level_two(side)
    gather.start_inplane(1)
    gather.start_inplane(0)
    now.forward(2)
    now.forward(3)
    now.inplane(-1)
    now.inplane(1)
    for side in range(2):
        gather.level_one(side)
    now.wait_far()
    for side in range(2):
        now.pick_out(side)
    now.out_two()
    now.inplane(-2)
    now.inplane(2)
    gather.level_zero()
    for load in loads[3:5]:
        load.wait()

    def update(e, rows, own_next):
        grad_sum = gather.total(e, rows)
        first_full = beta_one * first[e, rows].astype(jnp.float32) + (1.0 - beta_one) * grad_sum
        second_full = (
            beta_two * second[e, rows].astype(jnp.float32)
            + (1.0 - beta_two) * grad_sum * grad_sum
        )
        moved = master[e, rows] - learn_rate * (first_full / fix_one) / (
            jnp.sqrt(second_full / fix_two) + adam_eps
        )
        master[e, rows] = moved
        own_next[e] = moved.astype(jnp.bfloat16)
        first[e, rows] = first_full.astype(jnp.bfloat16)
        second[e, rows] = second_full.astype(jnp.bfloat16)
        return 0

    for at, part in enumerate(after):
        rows_at = pl.ds(*PARTS[at])
        lax.fori_loop(
            0, EXPERTS, lambda e, _, rows_at=rows_at, part=part: update(e, rows_at, part.own), 0
        )
        part.start_own(0)
    for part in after:
        part.inplane(0)
    for part in after:
        part.forward(0)
        part.inplane(-1)
        part.inplane(1)
    now.out_one()
    for part in after:
        part.wait_far()
        for side in range(2):
            part.pick_out(side)
        part.inplane(-2)
        part.inplane(2)
        part.out_two()
        part.out_one()
    for k in range(-3, 5):
        now.arrived(k)

    def back(block, _):
        at = pl.ds(pl.multiple_of(block * BLOCK, BLOCK), BLOCK)
        prod = lax.dot_general(
            cot[at, :], weight[...], (((1,), (1,)), ((), ())), preferred_element_type=jnp.float32
        )
        factor = gate[at, :]
        across = jnp.zeros((BLOCK, BLOCK), jnp.float32)
        for c in range(FF // BLOCK):
            part = prod[:, c * BLOCK : (c + 1) * BLOCK]
            cols = pl.ds(c * BLOCK, BLOCK)
            input_grad[at, cols] = (factor * part).astype(jnp.bfloat16)
            across = across + rows[at, cols].astype(jnp.float32) * part
        column = jnp.sum(across, axis=1, keepdims=True)
        turned = jnp.transpose(jnp.broadcast_to(column, (BLOCK, BLOCK)))
        gate_grad[pl.ds(block, 1), :] = turned[0:1, :]
        return 0

    lax.fori_loop(0, ROWS // BLOCK, back, 0)
    now.sent()
    gather.finish()
    for part in after:
        for k in range(-3, 5):
            part.arrived(k)
        part.sent()


def last_kernel(
    rows_next,
    weight,
    master,
    first,
    second,
    input_grad,
    gate_grad,
    next_out,
    master_out,
    first_out,
    second_out,
    input_out,
    gate_out,
    out,
    sems,
):
    pairs = (
        (master, master_out),
        (first, first_out),
        (second, second_out),
        (input_grad, input_out),
        (gate_grad, gate_out),
    )
    stores = [pltpu.make_async_copy(src, dst, sems.at[at]) for at, (src, dst) in enumerate(pairs)]
    for store in stores:
        store.start()
    for block in range(ROWS // BLOCK):
        at = pl.ds(block * BLOCK, BLOCK)
        out[at, :] = jnp.dot(
            rows_next[at, :], weight[...], preferred_element_type=jnp.float32
        ).astype(jnp.bfloat16)
        stores.append(
            pltpu.make_async_copy(out.at[at], next_out.at[at], sems.at[len(pairs) + block])
        )
        stores[-1].start()
    for store in stores:
        store.wait()


ANY = pl.BlockSpec(memory_space=pl.ANY)
HBM = pl.BlockSpec(memory_space=pltpu.HBM)
VMEM = pl.BlockSpec(memory_space=pltpu.VMEM)
SMEM = pl.BlockSpec(memory_space=pltpu.SMEM)


def in_hbm(x):
    return pltpu.with_memory_space_constraint(x, pltpu.HBM)


def step_call(*operands):
    return pl.pallas_call(
        step_kernel,
        out_shape=(
            jax.ShapeDtypeStruct((FF, D), jnp.bfloat16),
            jax.ShapeDtypeStruct(STATE, jnp.float32),
            jax.ShapeDtypeStruct(STATE, jnp.bfloat16),
            jax.ShapeDtypeStruct(STATE, jnp.bfloat16),
            jax.ShapeDtypeStruct((ROWS, FF), jnp.bfloat16),
            jax.ShapeDtypeStruct((ROWS // BLOCK, BLOCK), jnp.float32),
        ),
        in_specs=[SMEM] * 3 + [HBM] * 6,
        out_specs=(VMEM,) * 6,
        scratch_shapes=sum(SCRATCHES, []) + GATHER_SCRATCH + LOCAL_SCRATCH,
        compiler_params=pltpu.CompilerParams(
            has_side_effects=True, collective_id=0, vmem_limit_bytes=STEP_VMEM
        ),
    )(*operands)


STEP_VMEM = 39 * 2**20


def last_call(*operands):
    shapes = (
        jax.ShapeDtypeStruct((ROWS, D), jnp.bfloat16),
        jax.ShapeDtypeStruct(STATE, jnp.float32),
        jax.ShapeDtypeStruct(STATE, jnp.bfloat16),
        jax.ShapeDtypeStruct(STATE, jnp.bfloat16),
        jax.ShapeDtypeStruct((ROWS, FF), jnp.bfloat16),
        jax.ShapeDtypeStruct((ROWS // BLOCK, BLOCK), jnp.float32),
    )
    return pl.pallas_call(
        last_kernel,
        out_shape=shapes,
        in_specs=[VMEM] * 7,
        out_specs=(ANY,) * 6,
        scratch_shapes=[pltpu.VMEM((ROWS, D), jnp.bfloat16), pltpu.SemaphoreType.DMA((9,))],
        compiler_params=pltpu.CompilerParams(vmem_limit_bytes=16 * 2**20),
    )(*operands)


def shards(
    rows_in,
    cotangent,
    gate_prob,
    row_counts,
    old_place,
    new_place,
    rows_next,
    master,
    moment_one,
    moment_two,
):
    old, new = old_place.reshape(-1), new_place.reshape(-1)
    weight_next, new_master, new_first, new_second, input_grad, gate_grad = step_call(
        in_hbm(old),
        in_hbm(new),
        row_counts,
        in_hbm(gate_prob.reshape(ROWS // BLOCK, BLOCK)),
        in_hbm(rows_in),
        in_hbm(cotangent),
        in_hbm(master),
        in_hbm(moment_one),
        in_hbm(moment_two),
    )
    next_out, new_master, new_first, new_second, input_grad, gate_grad = last_call(
        rows_next, weight_next, new_master, new_first, new_second, input_grad, gate_grad
    )
    return (input_grad, gate_grad.reshape(-1), new_master, new_first, new_second, next_out)


def solution(mesh):
    in_specs = (
        P(("group", "slot"), None),
        P(("group", "slot"), None),
        P(("group", "slot")),
        P(("group", "slot")),
        P(),
        P(),
        P(("group", "slot"), None),
        P(None, "slot", "group"),
        P(None, "slot", "group"),
        P(None, "slot", "group"),
    )
    out_specs = (
        P(("group", "slot"), None),
        P(("group", "slot")),
        P(None, "slot", "group"),
        P(None, "slot", "group"),
        P(None, "slot", "group"),
        P(("group", "slot"), None),
    )
    return jax.shard_map(shards, mesh=mesh, in_specs=in_specs, out_specs=out_specs, check_vma=False)
```

```python
import jax
import jax.numpy as jnp
from jax import lax
from jax.experimental import pallas as pl
from jax.experimental.pallas import tpu as pltpu
from jax.sharding import PartitionSpec as P

beta_one = 0.9
beta_two = 0.999
adam_eps = 1e-08
learn_rate = 0.006
fix_one = 0.9999734386011124
fix_two = 0.0952078528862904

EXPERTS = 64
PR = 48
PC = 128
PLANES = 8
INPLANE = 32
FAR = 80
MESH = pl.DeviceIdType.MESH


def my_place():
    g = lax.axis_index("group")
    s = lax.axis_index("slot")
    z = lax.div(g, 2)
    return z, lax.rem(g, 2) * 16 + s, g, s


def plane_at(z, k):
    return lax.rem(z + (k + PLANES), PLANES)


def device_at(plane, i):
    return (plane * 2 + lax.div(i, 16), lax.rem(i, 16))


def each(count, go, first=0):
    _, _, g, s = my_place()
    for half in range(2):
        xlo = lax.rem(g + half, 2)

        def step(j, _, half=half, xlo=xlo):
            go(16 * half + j, xlo, lax.rem(s + j, 16))
            return 0

        lax.fori_loop(first if half == 0 else 0, count, step, 0)


def shard_slice(ref, block_row, block_col):
    return ref.at[
        pl.ds(pl.multiple_of(block_row * PR, 16), PR), pl.ds(pl.multiple_of(block_col * PC, PC), PC)
    ]


def send(src, dst, send_sem, recv_sem, device):
    copy = pltpu.make_async_remote_copy(
        src_ref=src,
        dst_ref=dst,
        send_sem=send_sem,
        recv_sem=recv_sem,
        device_id=device,
        device_id_type=MESH,
    )
    copy.start()


def take(ref, sem):
    pltpu.make_async_copy(ref, ref, sem).wait()


CHUNKS = 4
EARLY = 3
PARTS = ((0, 32), (32, 16))
PEERS = 5 * INPLANE - 1


def meet():
    z, _, g, s = my_place()
    barrier = pltpu.get_barrier_semaphore()
    for k in (2, -2, 1, -1, 0):
        for half in range(2):
            group = plane_at(z, k) * 2 + lax.rem(g + half, 2)

            def go(j, _, group=group):
                pl.semaphore_signal(
                    barrier,
                    inc=1,
                    device_id=(group, lax.rem(s + j, 16)),
                    device_id_type=MESH,
                )
                return 0

            lax.fori_loop(1 if (k, half) == (0, 0) else 0, 16, go, 0)
    return barrier


class Spread:
    def __init__(self, place, own, weight, first_row, chunks, bufs):
        self.place, self.own, self.weight = place, own, weight
        self.first_row, self.count = first_row, own.shape[1]
        self.chunks, self.step = chunks, EXPERTS // chunks
        self.near, self.far, self.picks = bufs[0:2], bufs[2:4], bufs[4]
        self.ring_sems, self.out_sem, self.in_sems = bufs[5:8]
        self.z, self.i, self.g, self.s = my_place()
        self.xlo = lax.rem(self.g, 2)

    def expert(self, plane, xlo, s):
        return self.place[plane * INPLANE + xlo * 16 + s]

    def ring(self, src, dst, hop, side, chunk):
        part = pl.ds(chunk * self.step, self.step)
        send(
            src.at[part],
            dst.at[part],
            self.ring_sems.at[0, hop, side, chunk],
            self.ring_sems.at[1, hop, side, chunk],
            device_at(plane_at(self.z, 1 - 2 * side), self.i),
        )

    def start_own(self, chunk):
        for side in range(2):
            self.ring(self.own, self.near[side], 0, side, chunk)

    def forward(self, chunk):
        for side in range(2):
            part = self.near[side].at[pl.ds(chunk * self.step, self.step)]
            take(part, self.ring_sems.at[1, 0, side, chunk])
            self.ring(self.near[side], self.far[side], 1, side, chunk)

    def wait_far(self):
        for chunk in range(self.chunks):
            for side in range(2):
                part = self.far[side].at[pl.ds(chunk * self.step, self.step)]
                take(part, self.ring_sems.at[1, 1, side, chunk])

    def span(self):
        return pl.ds(pl.multiple_of(self.s * PR + self.first_row, 16), self.count)

    def target(self, column):
        return self.weight.at[self.span(), pl.ds(pl.multiple_of(column * PC, PC), PC)]

    def inplane(self, k):
        z = self.z
        ref = {0: self.own, -1: self.near[0], 1: self.near[1], -2: self.far[0], 2: self.far[1]}[k]
        base = {0: 0, -1: 32, 1: 64, -2: 192, 2: 224}[k]
        column = plane_at(z, k) * 2 + self.xlo

        def pick(n, xlo, s):
            self.picks[base + n] = ref[self.expert(z, xlo, s)]

        def go(n, xlo, s):
            send(
                self.picks.at[base + n],
                self.target(column),
                self.out_sem,
                self.in_sems.at[k + 3],
                (z * 2 + xlo, s),
            )

        each(16, pick)
        each(16, go, 1)
        self.weight[self.span(), pl.ds(pl.multiple_of(column * PC, PC), PC)] = self.picks[base]

    def others(self, go):
        _, _, g, s = my_place()
        for half in range(2):
            xlo = lax.rem(g + half, 2)

            def step(j, _, half=half, xlo=xlo):
                go(8 * half + j, xlo, lax.rem(s - lax.rem(s, 2) + 2 * j, 16))
                return 0

            lax.fori_loop(0, 8, step, 0)

    def pick_out(self, side):
        ref, base = self.far[side], 96 + 48 * side
        sign = 1 - 2 * side
        one, two = plane_at(self.z, sign), plane_at(self.z, 2 * sign)

        def pick_two(n, xlo, s):
            self.picks[base + 32 + n] = ref[self.expert(two, xlo, s + side)]

        def pick_one(n, xlo, s):
            self.picks[base + n] = ref[self.expert(one, xlo, s)]

        self.others(pick_two)
        each(16, pick_one)

    def out_two(self):
        def go_two(n, xlo, s):
            for side in range(2):
                sign = 1 - 2 * side
                column = plane_at(self.z, -2 * sign) * 2 + self.xlo
                send(
                    self.picks.at[96 + 48 * side + 32 + n],
                    self.target(column),
                    self.out_sem,
                    self.in_sems.at[7],
                    (plane_at(self.z, 2 * sign) * 2 + xlo, s + side),
                )

        self.others(go_two)

    def out_one(self):
        def go_one(n, xlo, s):
            for side in range(2):
                sign = 1 - 2 * side
                column = plane_at(self.z, -2 * sign) * 2 + self.xlo
                send(
                    self.picks.at[96 + 48 * side + n],
                    self.target(column),
                    self.out_sem,
                    self.in_sems.at[3 - 3 * sign],
                    (plane_at(self.z, sign) * 2 + xlo, s),
                )

        each(16, go_one)

    def arrived(self, k):
        count = 31 if -2 <= k <= 2 else 32
        take(self.picks.at[pl.ds(0, count)], self.in_sems.at[k + 3])

    def sent(self):
        take(self.picks.at[pl.ds(0, 5 * 31 + 2 * 48)], self.out_sem)
        for chunk in range(self.chunks):
            for hop in range(2):
                for side in range(2):
                    part = self.own.at[pl.ds(chunk * self.step, self.step)]
                    take(part, self.ring_sems.at[0, hop, side, chunk])


def spread_scratch(rows, chunks):
    shards = [pltpu.VMEM((EXPERTS, rows, PC), jnp.bfloat16) for _ in range(4)]
    return shards + [
        pltpu.VMEM((256, rows, PC), jnp.bfloat16),
        pltpu.SemaphoreType.DMA((2, 2, 2, chunks)),
        pltpu.SemaphoreType.DMA,
        pltpu.SemaphoreType.DMA((8,)),
    ]


def build_tables(old, tab):
    z, _, _, _ = my_place()
    lanes = lax.broadcasted_iota(jnp.int32, (8, 128), 1)

    def near(t, lists):
        out = []
        for value, k in zip(lists, (-1, 1)):
            value = jnp.where(lanes == t, old[z * INPLANE + t], value)
            out.append(jnp.where(lanes == 32 + t, old[plane_at(z, k) * INPLANE + t], value))
        return tuple(out)

    def far(t, lists):
        out = []
        for core, (value, k) in enumerate(zip(lists, (-2, 2))):
            expert = old[plane_at(z, k) * INPLANE + 2 * t + core]
            out.append(jnp.where(lanes == 64 + t, expert, value))
        return tuple(out)

    none = jnp.full((8, 128), -1, jnp.int32)
    lists = lax.fori_loop(0, 16, far, lax.fori_loop(0, INPLANE, near, (none, none)))
    at = lax.broadcasted_iota(jnp.int32, (128, 128), 0)
    across = lax.broadcasted_iota(jnp.int32, (128, 128), 1)

    def put(row, found):
        value = jnp.where(found, at, -1)
        size = 128
        while size > 1:
            size //= 2
            value = jnp.maximum(value[:size], value[size:])
        tab[row : row + 1, :] = jnp.where(value < 0, FAR, value)

    for side in range(2):
        wide = jnp.broadcast_to(lists[side][0:1, :], (128, 128))
        tall = jnp.transpose(wide)
        put(side, (tall == wide) & (at < across))
        put(2 + side, tall == across)
        if side == 0:
            put(4, (tall == across) & (at < INPLANE))


class Gather:
    def __init__(self, tab, grad, met0, met1, met2, sums, parts, sems, part_sems):
        self.tab, self.grad = tab, grad
        self.met0, self.met1, self.met2 = met0, met1, met2
        self.sums = sums
        self.parts = parts
        self.sems, self.part_sems = sems, part_sems
        self.z, self.i, self.g, self.s = my_place()
        self.out_sem = sems.at[0]

    def piece(self, plane, xlo, s):
        return shard_slice(self.grad, s, plane * 2 + xlo)

    def piece_value(self, plane, t):
        rows = pl.ds(pl.multiple_of(lax.rem(t, 16) * PR, 16), PR)
        cols = pl.ds(pl.multiple_of((plane * 2 + lax.div(t, 16)) * PC, PC), PC)
        return self.grad[rows, cols]

    def start_far(self):
        z, i = self.z, self.i
        core = lax.rem(self.s, 2)
        two = lax.rem(z + 2 + 4 * core, PLANES)
        opposite = plane_at(z, 4)

        def go_two(n, xlo, s):
            send(
                self.piece(opposite, xlo, s),
                self.met2.at[core, 64 + lax.div(i, 2)],
                self.out_sem,
                self.sems.at[4 + core],
                (two * 2 + xlo, s),
            )

        def go_one(n, xlo, s):
            for side in range(2):
                sign = 1 - 2 * side
                send(
                    self.piece(plane_at(z, 3 * sign), xlo, s),
                    self.met2.at[side, 32 + i],
                    self.out_sem,
                    self.sems.at[4 + side],
                    (plane_at(z, sign) * 2 + xlo, s),
                )

        each(16, go_two)
        each(16, go_one)

    def start_inplane(self, level):
        z, i = self.z, self.i

        def go(n, xlo, s):
            for side in range(2):
                sign = 1 - 2 * side
                met = self.met2 if level == 2 else self.met1
                send(
                    self.piece(plane_at(z, level * sign), xlo, s),
                    met.at[side, i],
                    self.out_sem,
                    self.sems.at[2 * level + side],
                    (z * 2 + xlo, s),
                )

        def go_own(n, xlo, s):
            send(
                self.piece(z, xlo, s),
                self.met0.at[i],
                self.out_sem,
                self.sems.at[1],
                (z * 2 + xlo, s),
            )

        if level == 0:
            each(16, go_own, 1)
            self.met0[i] = self.piece_value(z, i)
            return
        each(16, go, 1)
        met = self.met2 if level == 2 else self.met1
        for side in range(2):
            met[side, i] = self.piece_value(plane_at(z, level * (1 - 2 * side)), i)

    def chain(self, value_at, count, row, sides):
        def step(t, _):
            for side in range(sides):
                before = self.sums[side][self.tab[row * side, t]]
                self.sums[side][t] = before + value_at(side, t).astype(jnp.float32)
            return 0

        lax.fori_loop(0, count, step, 0)

    def clear(self):
        for sums in self.sums:
            sums[...] = jnp.zeros_like(sums)

    def pass_on(self, level, side):
        sign = 1 - 2 * side
        send(
            self.parts[level].at[side],
            self.parts[2 + level].at[side],
            self.part_sems.at[0, level, side],
            self.part_sems.at[1, level, side],
            device_at(plane_at(self.z, sign), self.i),
        )

    def level_two(self):
        for side in range(2):
            take(self.met2.at[side, pl.ds(0, FAR - 1)], self.sems.at[4 + side])
        self.chain(lambda side, t: self.met2[side, t], FAR, 1, 2)

        def put(e, _):
            for side in range(2):
                value = self.sums[side][self.tab[2 + side, e]]
                self.parts[0][side, e] = value.astype(jnp.bfloat16)
            return 0

        lax.fori_loop(0, EXPERTS, put, 0)
        for side in range(2):
            self.pass_on(0, side)

    def level_one(self):
        for side in range(2):
            take(self.met1.at[side, pl.ds(0, INPLANE - 1)], self.sems.at[2 + side])
        self.chain(lambda side, t: self.met1[side, t], INPLANE, 0, 2)
        for side in range(2):
            take(self.parts[2].at[side], self.part_sems.at[1, 0, side])

        def put(e, _):
            for side in range(2):
                value = self.sums[side][self.tab[4, e]]
                value = value + self.parts[2][side, e].astype(jnp.float32)
                self.parts[1][side, e] = value.astype(jnp.bfloat16)
            return 0

        lax.fori_loop(0, EXPERTS, put, 0)
        for side in range(2):
            self.pass_on(1, side)

    def level_zero(self):
        take(self.met0.at[pl.ds(0, INPLANE - 1)], self.sems.at[1])
        self.chain(lambda _, t: self.met0[t], INPLANE, 0, 1)
        for side in range(2):
            take(self.parts[3].at[side], self.part_sems.at[1, 1, side])

    def total(self, e, rows):
        value = self.parts[3][0, e, rows].astype(jnp.float32)
        value = value + self.parts[3][1, e, rows].astype(jnp.float32)
        return value + self.sums[0][self.tab[4, e], rows]

    def finish(self):
        take(self.met2.at[0], self.out_sem)
        take(self.met2.at[0], self.out_sem)
        take(self.met2.at[0], self.out_sem)
        take(self.met2.at[0, pl.ds(0, 5 * 31 + 96 - 3 * FAR)], self.out_sem)
        for level in range(2):
            for side in range(2):
                take(self.parts[level].at[side], self.part_sems.at[0, level, side])


GATHER_SCRATCH = [
    pltpu.VMEM((INPLANE, PR, PC), jnp.bfloat16),
    pltpu.VMEM((2, INPLANE, PR, PC), jnp.bfloat16),
    pltpu.VMEM((2, FAR, PR, PC), jnp.bfloat16),
    pltpu.VMEM((FAR + 1, PR, PC), jnp.float32),
    pltpu.VMEM((FAR + 1, PR, PC), jnp.float32),
    pltpu.VMEM((2, EXPERTS, PR, PC), jnp.bfloat16),
    pltpu.VMEM((2, EXPERTS, PR, PC), jnp.bfloat16),
    pltpu.VMEM((2, EXPERTS, PR, PC), jnp.bfloat16),
    pltpu.VMEM((2, EXPERTS, PR, PC), jnp.bfloat16),
    pltpu.SemaphoreType.DMA((6,)),
    pltpu.SemaphoreType.DMA((2, 2, 2)),
]


STATE = (EXPERTS, PR, PC)
ROWS = 512
FF = 16 * PR
D = 16 * PC
BLOCK = 128
WIDE = 2 * PC
LOCAL_SCRATCH = [
    pltpu.VMEM(STATE, jnp.bfloat16),
    *[pltpu.VMEM((EXPERTS, rows, PC), jnp.bfloat16) for _, rows in PARTS],
    pltpu.VMEM((ROWS // BLOCK, BLOCK), jnp.float32),
    pltpu.VMEM((FF, D), jnp.bfloat16),
    pltpu.VMEM((FF, D), jnp.bfloat16),
    pltpu.VMEM((ROWS, FF), jnp.bfloat16),
    pltpu.VMEM((FF, ROWS), jnp.bfloat16),
    pltpu.VMEM((ROWS, D), jnp.bfloat16),
    pltpu.VMEM((ROWS, D), jnp.bfloat16),
    pltpu.VMEM((ROWS, BLOCK), jnp.float32),
    pltpu.SemaphoreType.DMA((7,)),
    pltpu.VMEM((8, 128), jnp.int32),
    pltpu.SMEM((8, 128), jnp.int32),
]


SCRATCHES = [spread_scratch(PR, CHUNKS)] + [spread_scratch(rows, 1) for _, rows in PARTS]

def step_kernel(
    old,
    new,
    count,
    gate_hbm,
    rows_in,
    cot_in,
    master_in,
    first_in,
    second_in,
    weight_next,
    master,
    first,
    second,
    input_grad,
    gate_grad,
    *scratch,
):
    n = len(SCRATCHES[0])
    m = len(GATHER_SCRATCH)
    own, own_a, own_b, gate_in, grad, weight, rows, rows_t, cot, scaled, gate, load_sems, tab, tab_smem = (
        scratch[3 * n + m :]
    )
    now = Spread(old, own, weight, 0, CHUNKS, scratch[0:n])
    after = [
        Spread(new, part, weight_next, PARTS[at][0], 1, scratch[(at + 1) * n : (at + 2) * n])
        for at, part in enumerate((own_a, own_b))
    ]
    rest = scratch[3 * n : 3 * n + m]
    gather = Gather(tab_smem, grad, *rest[0:3], rest[3:5], rest[5:9], *rest[9:])
    z = now.z

    barrier = meet()
    pairs = (
        (master_in, master),
        (rows_in, rows),
        (cot_in, cot),
        (first_in, first),
        (second_in, second),
        (gate_hbm, gate_in),
    )
    loads = [
        pltpu.make_async_copy(src, dst, load_sems.at[at]) for at, (src, dst) in enumerate(pairs)
    ]
    for load in loads:
        load.start()
    loads[0].wait()

    def cast(e, _):
        own[e] = master[e].astype(jnp.bfloat16)
        return 0

    lax.fori_loop(0, EXPERTS, cast, 0)
    pl.semaphore_wait(barrier, PEERS)
    for chunk in range(EARLY):
        now.start_own(chunk)

    now.inplane(0)
    build_tables(old, tab)
    loads[1].wait()
    loads[2].wait()
    loads[5].wait()
    live_count = count[0]
    for block in range(ROWS // BLOCK):
        at = pl.ds(block * BLOCK, BLOCK)
        live = lax.broadcasted_iota(jnp.int32, (BLOCK, BLOCK), 0) + block * BLOCK < live_count
        factor = jnp.transpose(jnp.broadcast_to(gate_in[block : block + 1, :], (BLOCK, BLOCK)))
        gate[at, :] = factor

        def mask_rows(c, _, at=at, live=live):
            cols = pl.ds(pl.multiple_of(c * BLOCK, BLOCK), BLOCK)
            value = jnp.where(live, rows[at, cols].astype(jnp.float32), 0.0)
            rows[at, cols] = value.astype(jnp.bfloat16)
            rows_t[cols, at] = jnp.transpose(value).astype(jnp.bfloat16)
            return 0

        def mask_cot(c, _, at=at, live=live, factor=factor):
            cols = pl.ds(pl.multiple_of(c * BLOCK, BLOCK), BLOCK)
            value = jnp.where(live, cot[at, cols].astype(jnp.float32), 0.0)
            cot[at, cols] = value.astype(jnp.bfloat16)
            scaled[at, cols] = (factor * value).astype(jnp.bfloat16)
            return 0

        lax.fori_loop(0, FF // BLOCK, mask_rows, 0)
        lax.fori_loop(0, D // BLOCK, mask_cot, 0)

    def slot_grad(p, _):
        half = lax.div(p + 1, 2)
        plane = lax.rem(z + 4 + (1 - 2 * lax.rem(p, 2)) * half, PLANES)
        cols = pl.ds(pl.multiple_of(plane * WIDE, WIDE), WIDE)
        grad[:, cols] = jnp.dot(
            rows_t[...], scaled[:, cols], preferred_element_type=jnp.float32
        ).astype(jnp.bfloat16)
        return 0

    lax.fori_loop(0, PLANES, slot_grad, 0)
    gather.clear()
    gather.start_far()
    for chunk in range(EARLY, CHUNKS):
        now.start_own(chunk)
    gather.start_inplane(2)
    tables = pltpu.make_async_copy(tab, tab_smem, load_sems.at[6])
    tables.start()
    tables.wait()
    now.forward(0)
    now.forward(1)
    gather.level_two()
    gather.start_inplane(1)
    gather.start_inplane(0)
    now.forward(2)
    now.forward(3)
    now.inplane(-1)
    now.inplane(1)
    gather.level_one()
    now.wait_far()
    for side in range(2):
        now.pick_out(side)
    now.out_two()
    now.inplane(-2)
    now.inplane(2)
    gather.level_zero()
    for load in loads[3:5]:
        load.wait()

    def update(e, rows, own_next):
        grad_sum = gather.total(e, rows)
        first_full = beta_one * first[e, rows].astype(jnp.float32) + (1.0 - beta_one) * grad_sum
        second_full = (
            beta_two * second[e, rows].astype(jnp.float32)
            + (1.0 - beta_two) * grad_sum * grad_sum
        )
        moved = master[e, rows] - learn_rate * (first_full / fix_one) / (
            jnp.sqrt(second_full / fix_two) + adam_eps
        )
        master[e, rows] = moved
        own_next[e] = moved.astype(jnp.bfloat16)
        first[e, rows] = first_full.astype(jnp.bfloat16)
        second[e, rows] = second_full.astype(jnp.bfloat16)
        return 0

    for at, part in enumerate(after):
        rows_at = pl.ds(*PARTS[at])
        lax.fori_loop(
            0, EXPERTS, lambda e, _, rows_at=rows_at, part=part: update(e, rows_at, part.own), 0
        )
        part.start_own(0)
    for part in after:
        part.inplane(0)
    for part in after:
        part.forward(0)
        part.inplane(-1)
        part.inplane(1)
    now.out_one()
    for part in after:
        part.wait_far()
        for side in range(2):
            part.pick_out(side)
        part.inplane(-2)
        part.inplane(2)
        part.out_two()
        part.out_one()
    for k in range(-3, 5):
        now.arrived(k)

    def back(block, _):
        at = pl.ds(pl.multiple_of(block * BLOCK, BLOCK), BLOCK)
        prod = lax.dot_general(
            cot[at, :], weight[...], (((1,), (1,)), ((), ())), preferred_element_type=jnp.float32
        )
        factor = gate[at, :]
        across = jnp.zeros((BLOCK, BLOCK), jnp.float32)
        for c in range(FF // BLOCK):
            part = prod[:, c * BLOCK : (c + 1) * BLOCK]
            cols = pl.ds(c * BLOCK, BLOCK)
            input_grad[at, cols] = (factor * part).astype(jnp.bfloat16)
            across = across + rows[at, cols].astype(jnp.float32) * part
        column = jnp.sum(across, axis=1, keepdims=True)
        turned = jnp.transpose(jnp.broadcast_to(column, (BLOCK, BLOCK)))
        gate_grad[pl.ds(block, 1), :] = turned[0:1, :]
        return 0

    lax.fori_loop(0, ROWS // BLOCK, back, 0)
    now.sent()
    gather.finish()
    for part in after:
        for k in range(-3, 5):
            part.arrived(k)
        part.sent()


def last_kernel(
    rows_next,
    weight,
    master,
    first,
    second,
    input_grad,
    gate_grad,
    next_out,
    master_out,
    first_out,
    second_out,
    input_out,
    gate_out,
    out,
    sems,
):
    pairs = (
        (master, master_out),
        (first, first_out),
        (second, second_out),
        (input_grad, input_out),
        (gate_grad, gate_out),
    )
    stores = [pltpu.make_async_copy(src, dst, sems.at[at]) for at, (src, dst) in enumerate(pairs)]
    for store in stores:
        store.start()
    for block in range(ROWS // BLOCK):
        at = pl.ds(block * BLOCK, BLOCK)
        out[at, :] = jnp.dot(
            rows_next[at, :], weight[...], preferred_element_type=jnp.float32
        ).astype(jnp.bfloat16)
        stores.append(
            pltpu.make_async_copy(out.at[at], next_out.at[at], sems.at[len(pairs) + block])
        )
        stores[-1].start()
    for store in stores:
        store.wait()


ANY = pl.BlockSpec(memory_space=pl.ANY)
HBM = pl.BlockSpec(memory_space=pltpu.HBM)
VMEM = pl.BlockSpec(memory_space=pltpu.VMEM)
SMEM = pl.BlockSpec(memory_space=pltpu.SMEM)


def in_hbm(x):
    return pltpu.with_memory_space_constraint(x, pltpu.HBM)


def step_call(*operands):
    return pl.pallas_call(
        step_kernel,
        out_shape=(
            jax.ShapeDtypeStruct((FF, D), jnp.bfloat16),
            jax.ShapeDtypeStruct(STATE, jnp.float32),
            jax.ShapeDtypeStruct(STATE, jnp.bfloat16),
            jax.ShapeDtypeStruct(STATE, jnp.bfloat16),
            jax.ShapeDtypeStruct((ROWS, FF), jnp.bfloat16),
            jax.ShapeDtypeStruct((ROWS // BLOCK, BLOCK), jnp.float32),
        ),
        in_specs=[SMEM] * 3 + [HBM] * 6,
        out_specs=(VMEM,) * 6,
        scratch_shapes=sum(SCRATCHES, []) + GATHER_SCRATCH + LOCAL_SCRATCH,
        compiler_params=pltpu.CompilerParams(
            has_side_effects=True, collective_id=0, vmem_limit_bytes=STEP_VMEM
        ),
    )(*operands)


STEP_VMEM = 41 * 2**20


def last_call(*operands):
    shapes = (
        jax.ShapeDtypeStruct((ROWS, D), jnp.bfloat16),
        jax.ShapeDtypeStruct(STATE, jnp.float32),
        jax.ShapeDtypeStruct(STATE, jnp.bfloat16),
        jax.ShapeDtypeStruct(STATE, jnp.bfloat16),
        jax.ShapeDtypeStruct((ROWS, FF), jnp.bfloat16),
        jax.ShapeDtypeStruct((ROWS // BLOCK, BLOCK), jnp.float32),
    )
    return pl.pallas_call(
        last_kernel,
        out_shape=shapes,
        in_specs=[VMEM] * 7,
        out_specs=(ANY,) * 6,
        scratch_shapes=[pltpu.VMEM((ROWS, D), jnp.bfloat16), pltpu.SemaphoreType.DMA((9,))],
        compiler_params=pltpu.CompilerParams(vmem_limit_bytes=16 * 2**20),
    )(*operands)


def shards(
    rows_in,
    cotangent,
    gate_prob,
    row_counts,
    old_place,
    new_place,
    rows_next,
    master,
    moment_one,
    moment_two,
):
    old, new = old_place.reshape(-1), new_place.reshape(-1)
    weight_next, new_master, new_first, new_second, input_grad, gate_grad = step_call(
        in_hbm(old),
        in_hbm(new),
        row_counts,
        in_hbm(gate_prob.reshape(ROWS // BLOCK, BLOCK)),
        in_hbm(rows_in),
        in_hbm(cotangent),
        in_hbm(master),
        in_hbm(moment_one),
        in_hbm(moment_two),
    )
    next_out, new_master, new_first, new_second, input_grad, gate_grad = last_call(
        rows_next, weight_next, new_master, new_first, new_second, input_grad, gate_grad
    )
    return (input_grad, gate_grad.reshape(-1), new_master, new_first, new_second, next_out)


def solution(mesh):
    in_specs = (
        P(("group", "slot"), None),
        P(("group", "slot"), None),
        P(("group", "slot")),
        P(("group", "slot")),
        P(),
        P(),
        P(("group", "slot"), None),
        P(None, "slot", "group"),
        P(None, "slot", "group"),
        P(None, "slot", "group"),
    )
    out_specs = (
        P(("group", "slot"), None),
        P(("group", "slot")),
        P(None, "slot", "group"),
        P(None, "slot", "group"),
        P(None, "slot", "group"),
        P(("group", "slot"), None),
    )
    return jax.shard_map(shards, mesh=mesh, in_specs=in_specs, out_specs=out_specs, check_vma=False)
```
